32 devices in a mesh: rep: 2 (over z, core), dp: 16 (over x, y).
Axes of the slice: x: 4, y: 4, z: 1, core: 2. Of those that a mesh axis runs over, the one named last changes fastest.
The devices are a block of a 4x4x8 slice.
Arguments:
- x: bfloat16 [32, 2048, 768], P(('rep', 'dp')), parts along dimension 0
- dy: bfloat16 [32, 2048, 768], P(('rep', 'dp')), parts along dimension 0
- wq: bfloat16 [2, 768, 768], replicated
- wk: bfloat16 [2, 768, 128], replicated
- wv: bfloat16 [2, 768, 128], replicated
- wo: bfloat16 [2, 768, 768], replicated
- w_gate: bfloat16 [2, 768, 2048], replicated
- w_up: bfloat16 [2, 768, 2048], replicated
- w_down: bfloat16 [2, 2048, 768], replicated
- m_wq: float32 [2, 768, 768], P(None, 'dp')
- m_wk: float32 [2, 768, 128], P(None, 'dp')
- m_wv: float32 [2, 768, 128], P(None, 'dp')
- m_wo: float32 [2, 768, 768], P(None, 'dp')
- m_w_gate: float32 [2, 768, 2048], P(None, 'dp')
- m_w_up: float32 [2, 768, 2048], P(None, 'dp')
- m_w_down: float32 [2, 2048, 768], P(None, 'dp')
- v_wq: float32 [2, 768, 768], P(None, 'dp')
- v_wk: float32 [2, 768, 128], P(None, 'dp')
- v_wv: float32 [2, 768, 128], P(None, 'dp')
- v_wo: float32 [2, 768, 768], P(None, 'dp')
- v_w_gate: float32 [2, 768, 2048], P(None, 'dp')
- v_w_up: float32 [2, 768, 2048], P(None, 'dp')
- v_w_down: float32 [2, 2048, 768], P(None, 'dp')
Outputs:
- output 1: bfloat16 [4, 768, 768], P('rep'), parts along dimension 0
- output 2: bfloat16 [4, 768, 128], P('rep'), parts along dimension 0
- output 3: bfloat16 [4, 768, 128], P('rep'), parts along dimension 0
- output 4: bfloat16 [4, 768, 768], P('rep'), parts along dimension 0
- output 5: bfloat16 [4, 768, 2048], P('rep'), parts along dimension 0
- output 6: bfloat16 [4, 768, 2048], P('rep'), parts along dimension 0
- output 7: bfloat16 [4, 2048, 768], P('rep'), parts along dimension 0
- output 8: float32 [4, 768, 768], P('rep', 'dp'), parts along dimension 0
- output 9: float32 [4, 768, 128], P('rep', 'dp'), parts along dimension 0
- output 10: float32 [4, 768, 128], P('rep', 'dp'), parts along dimension 0
- output 11: float32 [4, 768, 768], P('rep', 'dp'), parts along dimension 0
- output 12: float32 [4, 768, 2048], P('rep', 'dp'), parts along dimension 0
- output 13: float32 [4, 768, 2048], P('rep', 'dp'), parts along dimension 0
- output 14: float32 [4, 2048, 768], P('rep', 'dp'), parts along dimension 0
- output 15: float32 [4, 768, 768], P('rep', 'dp'), parts along dimension 0
- output 16: float32 [4, 768, 128], P('rep', 'dp'), parts along dimension 0
- output 17: float32 [4, 768, 128], P('rep', 'dp'), parts along dimension 0
- output 18: float32 [4, 768, 768], P('rep', 'dp'), parts along dimension 0
- output 19: float32 [4, 768, 2048], P('rep', 'dp'), parts along dimension 0
- output 20: float32 [4, 768, 2048], P('rep', 'dp'), parts along dimension 0
- output 21: float32 [4, 2048, 768], P('rep', 'dp'), parts along dimension 0
There are 2 independent parts. The reference program is written for one: setup_inputs(seed, part) draws one part's arguments, and reference() takes and returns one part's arrays. A program takes and returns all parts, laid end to end along the dimension named above; an argument that names none is the same for every part.
All inputs are finite; a program needn't handle non-finite values.
Results may differ from the reference program's by a relative error of at most 0.024.
Values are sent between devices in bfloat16 or wider.
A program may use at most 768 MiB of HBM per device.

```python
import jax
import jax.numpy as jnp
from jax import lax

SEQUENCES = 16
TOKENS = 2048
D = 768
HEADS = 6
KV_HEADS = 1
HEAD = 128
FF = 2048
LAYERS = 2
THETA = 10000
NAMES = ("wq", "wk", "wv", "wo", "w_gate", "w_up", "w_down")
SHAPES = {
    "wq": (LAYERS, D, HEADS * HEAD),
    "wk": (LAYERS, D, KV_HEADS * HEAD),
    "wv": (LAYERS, D, KV_HEADS * HEAD),
    "wo": (LAYERS, HEADS * HEAD, D),
    "w_gate": (LAYERS, D, FF),
    "w_up": (LAYERS, D, FF),
    "w_down": (LAYERS, FF, D),
}


def bump(key, n, height):
    away = (jnp.arange(n, dtype=jnp.int32) - jax.random.randint(key, (), 0, n, jnp.int32)) % n
    return jnp.where(away < n // 8, height, 1.0)


def together(key, own, strength):
    shared = jax.random.normal(key, own.shape[1:], jnp.float32)
    return (own + strength * shared) * lax.rsqrt(1 + strength * strength)


def setup_inputs(seed: int = 0, part: int = 0) -> dict:
    kx, kdy, ka, kb, kz, kf, kh, kl, *keys = jax.random.split(jax.random.key(seed), 8 + 3 * len(NAMES))
    kx, kdy, ka, kb = (jax.random.fold_in(k, part) for k in (kx, kdy, ka, kb))
    kw, km, kv = (keys[i::3] for i in range(3))
    shape = (SEQUENCES, TOKENS, D)
    much_x, much_dy = jax.random.uniform(kz, (2,), jnp.float32, 0.0, 1.0)
    loud = 2.0 ** jax.random.uniform(jax.random.fold_in(kz, 1), (), jnp.float32, -1.0, 2.0)
    layers = 2.0 ** jax.random.uniform(kl, (LAYERS, 1, 1), jnp.float32, -1.0, 1.0)
    times = {"wq": 1.0, "wk": 1.0, "wv": 2.0, "wo": layers, "w_gate": 1.0, "w_up": bump(kh, FF, 4.0), "w_down": layers}
    x = together(ka, jax.random.normal(kx, shape, jnp.float32), much_x) * bump(kf, D, 4.0)
    dy = together(kb, jax.random.normal(kdy, shape, jnp.float32), much_dy)
    drawn = {"x": x.astype(jnp.bfloat16), "dy": (loud * dy * (SEQUENCES * TOKENS) ** -0.5).astype(jnp.bfloat16)}
    for key, name in zip(kw, NAMES, strict=True):
        drawn[name] = (jax.random.normal(key, SHAPES[name], jnp.float32) * SHAPES[name][1] ** -0.5 * times[name]).astype(jnp.bfloat16)
    for key, name in zip(km, NAMES, strict=True):
        drawn[f"m_{name}"] = 0.1 * jax.random.normal(key, SHAPES[name], jnp.float32)
    for key, name in zip(kv, NAMES, strict=True):
        drawn[f"v_{name}"] = jax.random.uniform(key, SHAPES[name], jnp.float32, 0.02, 0.06)
    return drawn


def matmul(a, w):
    return jnp.dot(a, w, preferred_element_type=jnp.float32).astype(jnp.bfloat16)


def normed(h):
    wide = h.astype(jnp.float32)
    scale = lax.rsqrt(jnp.mean(wide**2, -1, keepdims=True) + 1e-6)
    return (wide * scale).astype(jnp.bfloat16)


def turned(t, theta):
    half = t.shape[-1] // 2
    angle = jnp.arange(t.shape[0], dtype=jnp.float32)[:, None] * theta ** (-jnp.arange(half, dtype=jnp.float32) / half)
    cos, sin = jnp.cos(angle)[:, None], jnp.sin(angle)[:, None]
    a, b = t[..., :half].astype(jnp.float32), t[..., half:].astype(jnp.float32)
    return jnp.concatenate([a * cos - b * sin, b * cos + a * sin], -1).astype(jnp.bfloat16)


def seen_by(q, k, v):
    tokens, kv = q.shape[0], k.shape[1]
    q = q.reshape(tokens, kv, -1, q.shape[-1])
    scores = jnp.einsum("tgsd,ugd->gstu", q.astype(jnp.float32), k.astype(jnp.float32)) * q.shape[-1] ** -0.5
    place = jnp.arange(tokens)
    weights = jax.nn.softmax(jnp.where(place[:, None] >= place, scores, -jnp.inf), -1).astype(jnp.bfloat16)
    return jnp.einsum("gstu,ugd->tgsd", weights.astype(jnp.float32), v.astype(jnp.float32)).astype(jnp.bfloat16).reshape(tokens, -1)


def layer(h, w):
    a = normed(h)
    q, k = (turned(matmul(a, w[name]).reshape(h.shape[0], -1, HEAD), THETA) for name in ("wq", "wk"))
    h = h + matmul(seen_by(q, k, matmul(a, w["wv"]).reshape(h.shape[0], -1, HEAD)), w["wo"])
    b = normed(h)
    gate = jnp.dot(b, w["w_gate"], preferred_element_type=jnp.float32)
    up = jnp.dot(b, w["w_up"], preferred_element_type=jnp.float32)
    return h + matmul((jax.nn.silu(gate) * up).astype(jnp.bfloat16), w["w_down"])


def adamw(w, m, v, g):
    m = 0.9 * m + 0.1 * g
    v = 0.95 * v + 0.05 * g * g
    step = m * lax.rsqrt(v + 1e-8) + 0.1 * w
    return (w - 0.02 * step).astype(jnp.bfloat16), m, v


def clipped(gradients, sum_of_squares, count):
    factor = jnp.minimum(1.0, 0.5 * lax.rsqrt(sum_of_squares / count + 1e-30))
    return [g * factor for g in gradients]


def stack(weights, h):
    return lax.scan(lambda h, w: (layer(h, w), None), h, weights)[0]


def reference(x, dy, wq, wk, wv, wo, w_gate, w_up, w_down, m_wq, m_wk, m_wv, m_wo, m_w_gate, m_w_up, m_w_down, v_wq, v_wk, v_wv, v_wo, v_w_gate, v_w_up, v_w_down):
    weights = dict(zip(NAMES, (wq, wk, wv, wo, w_gate, w_up, w_down), strict=True))

    def take(so_far, sequence):
        h, by_y = sequence
        _, back = jax.vjp(stack, weights, h)
        by_weights, by_h = back(by_y)
        return jax.tree.map(lambda total, term: total + term.astype(jnp.float32), so_far, by_weights), by_h

    none_yet = {name: jnp.zeros(w.shape, jnp.float32) for name, w in weights.items()}
    by_weights, by_x = lax.scan(take, none_yet, (x, dy))
    gradients = [by_weights[name].astype(jnp.bfloat16).astype(jnp.float32) for name in NAMES]
    gradients = clipped(gradients, sum(jnp.sum(g * g) for g in gradients), sum(g.size for g in gradients))
    first = (m_wq, m_wk, m_wv, m_wo, m_w_gate, m_w_up, m_w_down)
    second = (v_wq, v_wk, v_wv, v_wo, v_w_gate, v_w_up, v_w_down)
    new = [adamw(weights[name].astype(jnp.float32), m, v, g) for name, m, v, g in zip(NAMES, first, second, gradients, strict=True)]
    return tuple(one[which] for which in range(3) for one in new)
```

```python
import functools

import jax
import jax.numpy as jnp
from jax import lax
from jax.experimental import pallas as pl
from jax.experimental.pallas import tpu as pltpu
from jax.sharding import PartitionSpec as P

BF, F32 = jnp.bfloat16, jnp.float32
THETA = 10000
LOG2E = 1.4426950408889634
HIDDEN = -1e30
BOTH = range(2)
SIDES = 1, -1


FULL = 63 * 2**20
LANES = 128


MESH = pl.DeviceIdType.MESH
sd, vm, sem_of = jax.ShapeDtypeStruct, pltpu.VMEM, pltpu.SemaphoreType.DMA
any_ = pl.BlockSpec(memory_space=pl.ANY)


def remote(n):
    return dict(collective_id=n, has_side_effects=True)


def params(**more):
    return pltpu.CompilerParams(dimension_semantics=("arbitrary",), vmem_limit_bytes=FULL, **more)


def heads_block(heads, bm, d):
    return pl.BlockSpec((heads, bm, d), lambda i: (0, i, 0))


def stat_block(heads, bm):
    return pl.BlockSpec((heads, 1, bm), lambda i: (0, 0, i))


def on_first(run):
    pl.when(pl.program_id(0) == 0)(run)


def on_last(run):
    pl.when(pl.program_id(0) == pl.num_programs(0) - 1)(run)


def iota(shape, axis):
    return lax.broadcasted_iota(jnp.int32, shape, axis)


def lanes(n, size=LANES):
    return slice(n * size, n * size + size)


def dot(a, b, ca=1, cb=0):
    return lax.dot_general(a, b, (((ca,), (cb,)), ((), ())), preferred_element_type=F32)

def mm(a, b):
    return dot(a, b).astype(BF)


def dot_nt(a, b):
    return dot(a, b, 1, 1)


def dot_tn(a, b):
    return dot(a, b, 0, 0)

def sigmoid(g):
    return 1.0 / (1.0 + jnp.exp(-g))


def mean(x):
    return jnp.mean(x, -1, keepdims=True)


def top_of(x):
    return x.max(0, keepdims=True)


def norm_of(h):
    wide = h.astype(F32)
    scale = lax.rsqrt(mean(wide * wide) + 1e-6)
    return wide, scale, (wide * scale).astype(BF)

def norm_back(db, wide, scale):
    return scale * db - wide * (scale * scale * scale * mean(db * wide))

def turn(t, cos, sin):
    return t * cos + pltpu.roll(t, t.shape[1] // 2, 1) * sin

def tables(tokens, head, theta):
    half = head // 2
    rate = theta ** (-jnp.arange(half, dtype=F32) / half)
    low = 64
    a = (jnp.arange(tokens // low, dtype=F32) * low)[:, None] * rate
    b = jnp.arange(low, dtype=F32)[:, None] * rate
    ca, sa, cb, sb = (f(t) for t in (a, b) for f in (jnp.cos, jnp.sin))
    ca, sa, cb, sb = ca[:, None], sa[:, None], cb[None], sb[None]
    cos, sin = (ca * cb - sa * sb).reshape(tokens, half), (sa * cb + ca * sb).reshape(tokens, half)
    return jnp.concatenate([cos, cos], 1), jnp.concatenate([-sin, sin], 1)

def whole(a, layer=None):
    one = layer is not None
    return pl.BlockSpec((None,) * one + a.shape[one:], lambda *_: (layer,) * one + (0,) * (a.ndim - one), pipeline_mode=pl.Buffered(1))

def rows(bm, width):
    return pl.BlockSpec((bm, width), lambda i: (i, 0))

def heads_of(ref):
    return jnp.concatenate([ref[n] for n in range(ref.shape[0])], axis=1)

def project(a, wq, wk, wv, cos, sin, q_ref, k_ref, v_ref):
    hd = cos.shape[1]
    q = mm(a, wq).astype(F32)
    for n in range(q.shape[1] // hd):
        q_ref[n] = turn(q[:, lanes(n, hd)], cos, sin).astype(BF)
    k_ref[:] = turn(mm(a, wk).astype(F32), cos, sin).astype(BF)
    v_ref[:] = mm(a, wv)

def _pre(h_ref, cos_ref, sin_ref, wq, wk, wv, q_ref, k_ref, v_ref):
    _, _, a = norm_of(h_ref[:])
    project(a, wq[:], wk[:], wv[:], cos_ref[:], sin_ref[:], q_ref, k_ref, v_ref)

def pre(h, cos, sin, wq, wk, wv, layer, bm=512):
    t, d = h.shape
    hd = cos.shape[1]
    nh = wq.shape[2] // hd
    return pl.pallas_call(
        _pre, name="pre", grid=(t // bm,),
        in_specs=[rows(bm, d), rows(bm, hd), rows(bm, hd), whole(wq, layer), whole(wk, layer), whole(wv, layer)],
        out_specs=[heads_block(nh, bm, hd), rows(bm, hd), rows(bm, hd)],
        out_shape=[sd((nh, t, hd), BF), sd((t, hd), BF), sd((t, hd), BF)],
        compiler_params=params(),
    )(h, cos, sin, wq, wk, wv)

def fetch(pairs, sem):
    return [pltpu.make_async_copy(a, b, sem.at[n]) for n, (a, b) in enumerate(pairs)]

def _mid(o_ref, h_ref, cos_ref, sin_ref, wo, wg, wu, wd, wq, wk, wv, h1_ref, gu_ref, h2_ref, q_ref, k_ref, v_ref,
         wo_s, wg_s, wu_s, wd_s, wq_s, wk_s, wv_s, sem, *, layer, part):
    i = pl.program_id(0)
    cps = fetch([(a.at[layer], b) for a, b in ((wo, wo_s), (wg, wg_s), (wu, wu_s), (wd, wd_s))] +
                [(a.at[layer + 1], b) for a, b in ((wq, wq_s), (wk, wk_s), (wv, wv_s))], sem)

    @on_first
    def _():
        for c in cps: c.start()
        cps[0].wait()

    h1 = h_ref[:] + mm(heads_of(o_ref), wo_s[:])
    h1_ref[:] = h1
    _, _, b = norm_of(h1)

    @on_first
    def _():
        for c in cps[1:]: c.wait()

    f = wg_s.shape[1]
    y = None
    for at in range(0, f, part):
        c = slice(at, at + part)
        g, u = dot(b, wg_s[:, c]), dot(b, wu_s[:, c])
        gu_ref[:, c] = g
        gu_ref[:, f + at:f + at + part] = u
        act = (g * sigmoid(g) * u).astype(BF)
        yc = dot(act, wd_s[c, :])
        y = yc if y is None else y + yc
    h2 = h1 + y.astype(BF)
    h2_ref[:] = h2
    _, _, a = norm_of(h2)
    project(a, wq_s[:], wk_s[:], wv_s[:], cos_ref[:], sin_ref[:], q_ref, k_ref, v_ref)

def middle(o, h, cos, sin, wo, wg, wu, wd, wq, wk, wv, layer, bm=512, part=512):
    t, d = h.shape
    nh, _, hd = o.shape
    f = wg.shape[2]
    hs = heads_block(nh, bm, hd)
    return pl.pallas_call(
        functools.partial(_mid, layer=layer, part=part), name="middle", grid=(t // bm,),
        in_specs=[hs, rows(bm, d), rows(bm, hd), rows(bm, hd)] + [any_] * 7,
        out_specs=[rows(bm, d), rows(bm, 2 * f), rows(bm, d), hs, rows(bm, hd), rows(bm, hd)],
        out_shape=[sd((t, d), BF), sd((t, 2 * f), F32), sd((t, d), BF), sd((nh, t, hd), BF), sd((t, hd), BF), sd((t, hd), BF)],
        scratch_shapes=[vm(w.shape[1:], BF) for w in (wo, wg, wu, wd, wq, wk, wv)] + [sem_of((7,))],
        compiler_params=params(),
    )(o, h, cos, sin, wo, wg, wu, wd, wq, wk, wv)


class Square:
    def __init__(self, axis, side):
        self.axis, self.side = axis, side
        me = lax.axis_index(axis)
        self.me = me
        self.place = lax.div(me, side), lax.rem(me, side)

    def at(self, way, along, across=0):
        x, y = (lax.rem(p + (along if n == way else across) + self.side, self.side) for n, p in enumerate(self.place))
        return x * self.side + y

    def greet(self):
        for way in BOTH:
            for step in SIDES:
                pl.semaphore_signal(pltpu.get_barrier_semaphore(), device_id={self.axis: self.at(way, step)}, device_id_type=MESH)

    def met(self):
        pl.semaphore_wait(pltpu.get_barrier_semaphore(), 4)


class Ring:
    KINDS = "far", "free", "joined"

    def __init__(self, sq, way, send, keep, n, unit, s):
        self.sq, self.way, self.send, self.keep, self.unit = sq, way, send, keep, unit
        self.first, self.final, self.mid, self.own, self.out, self.send_sem, self.recv_sem, self.sem, self.own_sem = s
        cut = n // unit // 2 * unit
        self.halves = (0, cut), (cut, n - cut)
        self.n = n

    @staticmethod
    def scratch(k, n, unit, kept):
        most = n - n // unit // 2 * unit
        part, full = (len(BOTH), k, most, LANES), (k, n, LANES)
        return [vm(part, BF), vm((len(BOTH), *full), BF), vm(part, kept), vm(full, kept), vm(part, BF)] + [sem_of((3, len(BOTH)))] * 2 + [sem_of((len(BOTH),)), sem_of(())]

    def block(self, step):
        return lax.rem(self.sq.place[self.way] + step + self.sq.side, self.sq.side)

    def copy(self, kind, d):
        half = 1 - d if kind == "free" else d
        rows, size = pl.ds(*self.halves[half]), pl.ds(0, self.halves[half][1])
        src = self.out.at[d, :, size] if kind == "joined" else self.send(self.block(2 if kind == "far" else SIDES[d]), rows)
        dst = self.first.at[d, :, size] if kind == "far" else self.final.at[d, :, rows]
        n = self.KINDS.index(kind), d
        to = {self.sq.axis: self.sq.at(self.way, SIDES[d])}
        return pltpu.make_async_remote_copy(src, dst, self.send_sem.at[n], self.recv_sem.at[n], device_id=to, device_id_type=MESH)

    def added(self, d):
        rows, size = pl.ds(*self.halves[d]), self.halves[d][1]
        return pltpu.make_async_copy(self.keep(self.block(SIDES[d]), rows), self.mid.at[d, :, pl.ds(0, size)], self.sem.at[d])

    def mine(self):
        return pltpu.make_async_copy(self.keep(self.block(0), pl.ds(0, self.n)), self.own, self.own_sem)

    def start(self):
        for kind in self.KINDS[:2]:
            for d in BOTH:
                self.copy(kind, d).start()
        for d in BOTH:
            self.added(d).start()
        self.mine().start()

    def steps(self, size, run):
        def body(t, _):
            run(pl.ds(pl.multiple_of(t * self.unit, self.unit), self.unit))
            return _

        lax.fori_loop(0, size // self.unit, body, 0)

    def middle(self):
        for d in BOTH:
            self.copy("far", d).wait_recv()
            self.added(d).wait()

            def add(here, d=d):
                self.out[d, :, here] = (self.mid[d, :, here].astype(F32) + self.first[d, :, here].astype(F32)).astype(BF)

            self.steps(self.halves[d][1], add)
            self.copy("joined", d).start()

    def finish(self, put):
        for d in BOTH:
            for kind in self.KINDS[1:]:
                self.copy(kind, d).wait_recv()
        self.mine().wait()
        self.steps(self.n, lambda here: put(here, self.own[:, here].astype(F32) + sum(self.final[d, :, here].astype(F32) for d in BOTH)))
        for d in BOTH:
            for kind in self.KINDS:
                self.copy(kind, d).wait_send()


def first_rings(sq, g, unit, scr):
    n = g.shape[2] // 2
    x_block = lambda p, rows: g.at[p, :, rows]
    y_block = lambda p, rows: g.at[:, p, pl.ds(rows.start + n, rows.size)]
    return [Ring(sq, way, block, block, n, unit, scr[way]) for way, block in enumerate((x_block, y_block))]


def second_rings(sq, wide, low, unit, scr):
    pick = lambda ref, way: (lambda p, rows: ref.at[way, pl.ds(p, 1), rows])
    return [Ring(sq, 1 - way, pick(low, way), pick(wide, way), wide.shape[2], unit, scr[way]) for way in BOTH]


def ring_scratch(k, n, unit, kept):
    return Ring.scratch(k, n // 2, unit, kept) * 2


def pairs(scr):
    half = len(scr) // 2
    return scr[:half], scr[half:]


def keeper(way, wide, low):
    def put(rows, total):
        wide[way, :, rows] = total
        low[way, :, rows] = total.astype(BF)
    return put


def rounder(way, g, n, at=0):
    def put(rows, total):
        g[pl.ds(pl.multiple_of(rows.start + (at + way * n), 16), rows.size)] = total[0].astype(BF)
    return put


def leave(sq, way, ring, low, wide, sem):
    q, side = sq.place[1 - way], sq.side
    full, (one, other) = pl.ds(0, ring.n), (pl.ds(*h) for h in ring.halves)
    got = []
    for pair, parts in ((wide, (full, one, None, other)), (low, (None, other, full, one))):
        for step, part in enumerate(parts):
            if part:
                at = way, lax.rem(q + step, side), part
                got.append(pltpu.make_async_copy(pair[0].at[at], pair[1].at[at], sem.at[len(got)]))
                got[-1].start()
    return got


def _attend(q_ref, k_ref, v_ref, o_ref, lse_ref, s_a, s_b, top_a, top_b, vt_s, gap_s, *, scale, bq):
    heads, _, d = q_ref.shape
    tokens = k_ref.shape[0]
    iq = pl.program_id(0)
    e = scale * LOG2E

    @on_first
    def _():
        vt_s[:d, :] = v_ref[:].astype(F32).T.astype(BF)
        vt_s[d:, :] = jnp.ones_like(vt_s[d:, :])
        gap_s[:] = iota(gap_s.shape, 1) - iota(gap_s.shape, 0)

    half = bq // 2

    def score(n, keys, s_ref, top_ref):
        q = q_ref[n]
        cut = keys - half
        top = None
        if keys > bq:
            s = dot_nt(k_ref[:keys - bq, :], q)
            s_ref[:keys - bq, :] = s
            top = top_of(s)
        near = dot_nt(k_ref[keys - bq:cut, :], q)
        left = jnp.where(gap_s[:] >= 0, near[:, :half], HIDDEN)
        right = near[:, half:]
        s_ref[keys - bq:cut, :half] = left
        s_ref[keys - bq:cut, half:] = right
        far = jnp.where(gap_s[:] >= 0, dot_nt(k_ref[cut:keys, :], q[half:, :]), HIDDEN)
        s_ref[cut:keys, half:] = far
        m = jnp.concatenate([top_of(left), jnp.maximum(top_of(right), top_of(far))], 1)
        top_ref[:] = m if top is None else jnp.maximum(m, top)

    def weigh(n, keys, s_ref, top_ref):
        cut = keys - half
        top = top_ref[:]
        pa = jnp.exp2((s_ref[:cut, :] - top) * e).astype(BF)
        pb = jnp.exp2((s_ref[cut:keys, half:] - top[:, half:]) * e).astype(BF)
        mix = dot(vt_s[:, :cut], pa)
        more = dot(vt_s[:, cut:keys], pb)
        mix = jnp.concatenate([mix[:, :half], mix[:, half:] + more], 1)
        total = mix[d:d + 1, :]
        o_ref[n] = (mix[:d, :] * (1.0 / total)).T.astype(o_ref.dtype)
        lse_ref[n] = top * scale + jnp.log(total)

    for j in range(tokens // bq):
        @pl.when(iq == j)
        def _(keys=(j + 1) * bq):
            score(0, keys, s_a, top_a)

            def pair(t, _):
                score(2 * t + 1, keys, s_b, top_b)
                weigh(2 * t, keys, s_a, top_a)
                score(2 * t + 2, keys, s_a, top_a)
                weigh(2 * t + 1, keys, s_b, top_b)
                return _

            lax.fori_loop(0, heads // 2 - 1, pair, 0)
            score(heads - 1, keys, s_b, top_b)
            weigh(heads - 2, keys, s_a, top_a)
            weigh(heads - 1, keys, s_b, top_b)

def attend(q, k, v, scale, bq=512):
    heads, tokens, d = q.shape
    here = heads_block(heads, bq, d)
    all_ = whole(k)
    return pl.pallas_call(
        functools.partial(_attend, scale=scale, bq=bq), name="attend", grid=(tokens // bq,),
        in_specs=[here, all_, all_],
        out_specs=[here, stat_block(heads, bq)],
        out_shape=[sd(q.shape, BF), sd((heads, 1, tokens), F32)],
        scratch_shapes=[vm((tokens, bq), F32), vm((tokens, bq), F32), vm((1, bq), F32), vm((1, bq), F32),
                        vm((d + 8, tokens), BF), vm((bq // 2, bq // 2), jnp.int32)],
        compiler_params=params(),
    )(q, k, v)
def _attend_back(q_ref, k_ref, v_ref, do_ref, lse_ref, delta_ref, g_ref, dq_ref, dk_ref, dv_ref, wide_ref, low_ref,
                 s_a, s_b, dp_a, dp_b, kt_s, vt_s, dkt_s, dvt_s, gap_s, wide_s, low_s, out_sem, *scr, scale, bq, side, axis, unit):
    heads, _, d = q_ref.shape
    tokens = k_ref.shape[0]
    iq = pl.program_id(0)
    e = scale * LOG2E
    half = bq // 2

    sq = Square(axis, side)
    rings = first_rings(sq, g_ref, unit, pairs(scr))
    last = pl.num_programs(0) - 1

    @on_first
    def _():
        sq.greet()
        row = iota((d, tokens), 0)
        kt_s[:d, :] = k_ref[:].astype(F32).T.astype(BF)
        kt_s[d:, :] = jnp.where(row < 3, 1.0, 0.0).astype(BF)
        vt_s[:d, :] = v_ref[:].astype(F32).T.astype(BF)
        vt_s[d:, :] = jnp.where((row >= 3) & (row < 6), 1.0, 0.0).astype(BF)
        gap_s[:] = iota(gap_s.shape, 0) - iota(gap_s.shape, 1)
        dkt_s[:] = jnp.zeros_like(dkt_s)
        dvt_s[:] = jnp.zeros_like(dvt_s)
        sq.met()
        for r in rings: r.start()

    @on_last
    def _():
        for r in rings: r.middle()

    def parts(x):
        a = x.astype(BF).astype(F32)
        b = (x - a).astype(BF).astype(F32)
        return [a, b, x - a - b]

    def score(n, keys, s_ref, dp_ref):
        cut = keys - half
        row = iota((d, bq), 0)
        rows = jnp.zeros((d, bq), F32)
        for i, x in enumerate(parts(lse_ref[n] * (-1 / scale)) + parts(-delta_ref[n])):
            rows = jnp.where(row == i, x, rows)
        extra = rows.T.astype(BF)
        q = jnp.concatenate([q_ref[n], extra], 1)
        do = jnp.concatenate([do_ref[n], extra], 1)
        if keys > bq:
            s_ref[:, :keys - bq] = dot(q, kt_s[:, :keys - bq])
        near = dot(q, kt_s[:, keys - bq:cut])
        s_ref[:half, keys - bq:cut] = jnp.where(gap_s[:] >= 0, near[:half], HIDDEN)
        s_ref[half:, keys - bq:cut] = near[half:]
        s_ref[half:, cut:keys] = jnp.where(gap_s[:] >= 0, dot(q[half:], kt_s[:, cut:keys]), HIDDEN)
        dp_ref[:, :cut] = dot(do, vt_s[:, :cut])
        dp_ref[half:, cut:keys] = dot(do[half:], vt_s[:, cut:keys])

    def weigh(n, keys, s_ref, dp_ref):
        cut = keys - half
        qt = q_ref[n].astype(F32).T.astype(BF)
        dot_ = do_ref[n].astype(F32).T.astype(BF)
        pa = jnp.exp2(s_ref[:, :cut] * e)
        da = (pa * dp_ref[:, :cut]).astype(BF)
        pb = jnp.exp2(s_ref[half:, cut:keys] * e)
        db = (pb * dp_ref[half:, cut:keys]).astype(BF)
        dvt_s[:, :cut] += dot(dot_, pa.astype(BF))
        dkt_s[:, :cut] += dot(qt, da)
        dvt_s[:, cut:keys] += dot(dot_[:, half:], pb.astype(BF))
        dkt_s[:, cut:keys] += dot(qt[:, half:], db)
        dq = dot(da, k_ref[:cut, :])
        far = dot(db, k_ref[cut:keys, :])
        dq_ref[n, :half] = (dq[:half] * scale).astype(BF)
        dq_ref[n, half:] = ((dq[half:] + far) * scale).astype(BF)

    for j in range(tokens // bq):
        @pl.when(iq == j)
        def _(keys=(j + 1) * bq):
            score(0, keys, s_a, dp_a)

            def pair(t, _):
                score(2 * t + 1, keys, s_b, dp_b)
                weigh(2 * t, keys, s_a, dp_a)
                score(jnp.minimum(2 * t + 2, heads - 1), keys, s_a, dp_a)
                weigh(2 * t + 1, keys, s_b, dp_b)
                return _

            lax.fori_loop(0, heads // 2, pair, 0)

    @on_last
    def _():
        outs = []
        for way, r in enumerate(rings):
            r.finish(keeper(way, wide_s, low_s))
            outs += leave(sq, way, r, (low_s, low_ref), (wide_s, wide_ref), out_sem.at[way])
        dk_ref[:] = (dkt_s[:] * scale).T.astype(BF)
        dv_ref[:] = dvt_s[:].T.astype(BF)
        for c in outs: c.wait()

def attend_back(q, k, v, do, lse, delta, scale, g, side, axis, unit, bq=512):
    n = g.shape[2]
    half = (2, side, n // 2, LANES)
    heads, tokens, d = q.shape
    here = heads_block(heads, bq, d)
    all_ = whole(k)
    stat = stat_block(heads, bq)
    return pl.pallas_call(
        functools.partial(_attend_back, scale=scale, bq=bq, side=side, axis=axis, unit=unit), name="attend_back", grid=(tokens // bq,),
        in_specs=[here, all_, all_, here, stat, stat, any_],
        out_specs=[here, all_, all_, any_, any_],
        out_shape=[sd(q.shape, BF)] + [sd(k.shape, BF)] * 2 + [sd(half, F32), sd(half, BF)],
        scratch_shapes=[vm((bq, tokens), F32)] * 4 + [vm((2 * d, tokens), BF)] * 2 + [vm((d, tokens), F32)] * 2 +
                       [vm((bq // 2, bq // 2), jnp.int32), vm(half, F32), vm(half, BF), sem_of((2, 6))] + ring_scratch(side, n, unit, BF),
        compiler_params=params(**remote(1)),
    )(q, k, v, do, lse, delta, g)


def split_rows(x, side, r):
    return x.astype(BF).reshape(side, side, r, x.shape[1])


def put_columns(acc, stage, at, side):
    r = acc.shape[0] // (side * side)
    for cb in range(acc.shape[1] // LANES):
        stage[:, :, at:at + r, :] = split_rows(acc[:, lanes(cb)], side, r)
        at += r
    return at


def sync(a, b, sem):
    c = pltpu.make_async_copy(a, b, sem.at[0])
    c.start()
    c.wait()


def copy_rows(stage, out, at, sem):
    c = pltpu.make_async_copy(stage, out.at[:, :, pl.ds(at, stage.shape[2])], sem)
    c.start()
    return c


def mlp_body(i, o, h1, dy, gu, w, acc, dh_ref, do_ref, delta_ref, part):
    wo_s, wg_s, wu_s, wd_s = w
    dwg_s, dwu_s, dwd_s, dwo_s = acc
    heads, _, hd = do_ref.shape
    wide, scale, b = norm_of(h1)
    db = None
    for at in range(0, wg_s.shape[1], part):
        c = slice(at, at + part)
        g, u = gu(c) if gu else (dot(b, wg_s[:, c]), dot(b, wu_s[:, c]))
        da = dot_nt(dy, wd_s[c, :]).astype(BF).astype(F32)
        s = sigmoid(g)
        silu = g * s
        act = (silu * u).astype(BF)
        du = (da * silu).astype(BF)
        dg = (da * u * (s + silu * (1.0 - s))).astype(BF)
        dbc = dot_nt(dg, wg_s[:, c]) + dot_nt(du, wu_s[:, c])
        db = dbc if db is None else db + dbc
        dwg_s[:, c] += dot_tn(b, dg)
        dwu_s[:, c] += dot_tn(b, du)
        dwd_s[:, c] += dot_tn(dy, act)
    dh = dy + norm_back(db.astype(BF).astype(F32), wide, scale).astype(BF)
    dh_ref[:] = dh
    do = dot_nt(dh, wo_s[:]).astype(BF)
    prod = do.astype(F32) * o.astype(F32)
    lane = iota((dy.shape[0], LANES), 1)
    table = jnp.zeros((dy.shape[0], LANES), F32)
    for n in range(heads):
        c = lanes(n, hd)
        do_ref[n] = do[:, c]
        table = jnp.where(lane == n, jnp.sum(prod[:, c], -1, keepdims=True), table)
    table = table.T
    for n in range(heads):
        delta_ref[n] = table[n:n + 1, :]
    dwo_s[:] += dot_tn(o, dh)


def _mlp_back(*refs, layer, part, side, axis, kept):
    i, steps = pl.program_id(0), pl.num_programs(0)
    o_ref, h_ref, dy_ref, *refs = refs
    if kept:
        gu_ref, *refs = refs
    wo, wg, wu, wd, *refs = refs
    if kept:
        early, *refs = refs
    dh_ref, do_ref, delta_ref, big, small, *refs = refs
    if kept:
        g_out, *refs = refs
    wo_s, wg_s, wu_s, wd_s, dwg_s, dwu_s, dwd_s, dwo_s, st_a, st_b, sem, sem_a, sem_b, *refs = refs
    w, acc = (wo_s, wg_s, wu_s, wd_s), (dwg_s, dwu_s, dwd_s, dwo_s)
    cps = [pltpu.make_async_copy(a.at[layer], b, sem.at[n]) for n, (a, b) in enumerate(zip((wo, wg, wu, wd), w))]
    if kept:
        wide_s, low_s, g_s, *scr = refs
        sq = Square(axis, side)
        unit = dh_ref.shape[1] // (side * side)
        half = len(scr) // 2
        one = first_rings(sq, early, unit, pairs(scr[:half]))
        two = second_rings(sq, wide_s, low_s, unit, pairs(scr[half:]))

    @on_first
    def _():
        for c in cps: c.start()
        if kept: sq.greet()
        for r in acc: r[:] = jnp.zeros_like(r)
        if kept:
            sq.met()
            for r in one: r.start()
        for c in cps: c.wait()

    if kept:
        @pl.when(i == steps // 2 - 1)
        def _():
            for r in one: r.middle()

        @pl.when(i == steps // 2 + 1)
        def _():
            for way, r in enumerate(one): r.finish(keeper(way, wide_s, low_s))
            for r in two: r.start()

        @on_last
        def _():
            for r in two: r.middle()

    o, dy = heads_of(o_ref), dy_ref[:]
    if kept:
        f = gu_ref.shape[1] // 2
        mlp_body(i, o, h_ref[:], dy, lambda c: (gu_ref[:, c], gu_ref[:, c.start + f:c.stop + f]), w, acc, dh_ref, do_ref, delta_ref, part)
    else:
        mlp_body(i, o, h_ref[:] + mm(o, wo_s[:]), dy, None, w, acc, dh_ref, do_ref, delta_ref, part)

    @on_last
    def _():
        n = st_a.shape[2]
        put_columns(dwg_s, st_a, 0, side)
        first = copy_rows(st_a, big, 0, sem_a)
        put_columns(dwu_s, st_b, 0, side)
        second = copy_rows(st_b, big, n, sem_b)
        first.wait()
        for x in range(side):
            for y in range(side):
                st_a[x, y] = dwd_s[:, lanes(x * side + y)].astype(BF)
        third = copy_rows(st_a, big, 2 * n, sem_a)
        second.wait()
        size = put_columns(dwo_s, st_b, 0, side)
        fourth = copy_rows(st_b.at[:, :, pl.ds(0, size)], small, 0, sem_b)
        if kept:
            for way, r in enumerate(two): r.finish(rounder(way, g_s, r.n))
            sync(g_s, g_out, sem)
        third.wait()
        fourth.wait()


def mlp_back(o, h, dy, wo, wg, wu, wd, layer, side, axis, gu=None, early=None, bm=256, part=512):
    t, d = h.shape
    nh, _, hd = o.shape
    f = wg.shape[2]
    kept = gu is not None
    hs = heads_block(nh, bm, hd)
    unit = d // (side * side)
    n_big, n_small = 3 * d, (d // LANES + nh + 2) * unit
    given = [o, h, dy] + [gu] * kept + [wo, wg, wu, wd] + [early] * kept
    half = n_small // 2
    return pl.pallas_call(
        functools.partial(_mlp_back, layer=layer, part=part, side=side, axis=axis, kept=kept), name=f"mlp_back{layer}", grid=(t // bm,),
        in_specs=[hs, rows(bm, d), rows(bm, d)] + [rows(bm, 2 * f)] * kept + [any_] * (4 + kept),
        out_specs=[rows(bm, d), hs, stat_block(nh, bm)] + [any_] * (2 + kept),
        out_shape=[sd((t, d), BF), sd((nh, t, hd), BF), sd((nh, 1, t), F32), sd((side, side, n_big, LANES), BF), sd((side, side, n_small, LANES), BF)] +
                  [sd((n_small, LANES), BF)] * kept,
        scratch_shapes=[vm(w.shape[1:], BF) for w in (wo, wg, wu, wd)] + [vm((d, f), F32)] * 3 + [vm((d, d), F32)] + [vm((side, side, d, LANES), BF)] * 2 +
                       [sem_of((4,)), sem_of(()), sem_of(())] +
                       ([vm((2, side, half, LANES), F32), vm((2, side, half, LANES), BF), vm((n_small, LANES), BF)] +
                        ring_scratch(side, n_small, unit, BF) + ring_scratch(1, n_small, unit, F32) if kept else []),
        compiler_params=params(**(remote(3) if kept else {})),
    )(*given)


def _pre_back(*refs, layer, side, axis, deep):
    i, steps = pl.program_id(0), pl.num_programs(0)
    dq_ref, dk_ref, dv_ref, h_ref, cos_ref, sin_ref, *refs = refs
    if deep:
        dh_ref, wq, wk, wv, wide, low, _, out_dh, g_out, out, dw_s, stage, out_sem, sem, g_s, *refs = refs
        sq = Square(axis, side)
        rings = second_rings(sq, wide, low, h_ref.shape[1] // (side * side), pairs(refs))
    else:
        _, out, dw_s, stage, out_sem, _ = refs
    nh = dq_ref.shape[0]

    @on_first
    def _():
        if deep: sq.greet()
        dw_s[:] = jnp.zeros_like(dw_s)
        if deep:
            sq.met()
            for r in rings: r.start()

    if deep:
        @pl.when(i == steps // 2)
        def _():
            for r in rings: r.middle()

    cos, sin = cos_ref[:], -sin_ref[:]
    wide_h, scale, a = norm_of(h_ref[:])
    ds = [turn(dq_ref[n].astype(F32), cos, sin).astype(BF) for n in range(nh)] + [turn(dk_ref[:].astype(F32), cos, sin).astype(BF), dv_ref[:]]
    dw_s[:] += dot_tn(a, jnp.concatenate(ds, 1))
    if deep:
        da = dot_nt(jnp.concatenate(ds[:nh], 1), wq[:]) + dot_nt(ds[nh], wk[:]) + dot_nt(ds[nh + 1], wv[:])
        out_dh[:] = dh_ref[:] + norm_back(da.astype(BF).astype(F32), wide_h, scale).astype(BF)

    @on_last
    def _():
        size = put_columns(dw_s, stage, 0, side)
        c = copy_rows(stage, out, out.shape[2] - size, out_sem)
        if deep:
            for way, r in enumerate(rings): r.finish(rounder(way, g_s, r.n))
            sync(g_s, g_out, sem)
        c.wait()


def pre_back(dq, dk, dv, h, cos, sin, layer, side, axis, small, deep=None, bm=512):
    t, d = h.shape
    nh, _, hd = dq.shape
    unit = d // (side * side)
    size = (nh + 2) * unit
    given = [dq, dk, dv, h, cos, sin, *(deep or ()), small]
    more, more_s, more_in = [], [], []
    if deep:
        n = deep[4].shape[2] * 2
        more = [sd((t, d), BF), sd((n, LANES), BF)]
        more_in = [rows(bm, d)] + [whole(w, layer) for w in deep[1:4]] + [any_] * 2
        more_s = [vm((n, LANES), BF)] + ring_scratch(1, n, unit, F32)
    return pl.pallas_call(
        functools.partial(_pre_back, layer=layer, side=side, axis=axis, deep=bool(deep)), name=f"pre_back{layer}", grid=(t // bm,),
        in_specs=[heads_block(nh, bm, hd), rows(bm, hd), rows(bm, hd), rows(bm, d), rows(bm, hd), rows(bm, hd)] + more_in + [any_],
        out_specs=([rows(bm, d), any_] if deep else []) + [any_],
        out_shape=more + [sd(small.shape, BF)],
        input_output_aliases={len(given) - 1: len(more)},
        scratch_shapes=[vm((d, (nh + 2) * hd), F32), vm((side, side, size, LANES), BF), sem_of(()), sem_of((1,))] + more_s,
        compiler_params=params(**(remote(2) if deep else {})),
    )(*given)


def segments(shapes, order, group):
    out, at = [], 0
    for i, l in order:
        r, c = shapes[i][1] // group, shapes[i][2]
        out.append((i, l, r, c, at))
        at += r * c // LANES
    return out, at


def moments(m, v, g):
    return 0.9 * m + 0.1 * g, 0.95 * v + 0.05 * g * g


def blocks_of(segs, begin, end):
    for i, l, r, c, at in segs:
        for cb in range(c // LANES):
            if begin <= at + cb * r < end:
                yield i, l, lanes(cb), at + cb * r, r


def sevens(refs, k=7):
    return [refs[i * k:i * k + k] for i in range(3)], refs[3 * k:]


class Gather:
    ALONG = 0, -1, 1, 2

    def __init__(self, sq, way, part, span, new, buf, send_sem, recv_sem):
        self.sq, self.way, self.part, self.new, self.buf, self.sems, self.sent = sq, way, part, new, buf, (send_sem, recv_sem), []
        begin, end = span
        mid = begin + (end - begin) // 32 * 16
        self.spans = (begin, end - begin), (begin, mid - begin), (mid, end - mid)

    def copy(self, m, source, to, which, own=False):
        along, across = source
        owner = self.sq.at(self.way, along, across)
        rows = pl.ds(*self.spans[which])
        place = self.buf.at[owner, rows]
        s, r = (x.at[self.part, *m] for x in self.sems)
        return pltpu.make_async_remote_copy(self.new.at[rows] if own else place, place, s, r, device_id={self.sq.axis: self.sq.at(self.way, *to)}, device_id_type=MESH)

    def go(self, *a, **k):
        c = self.copy(*a, **k)
        c.start()
        self.sent.append(c)

    def got(self, m, source, which):
        self.copy(m, source, (1, 0), which).wait_recv()

    def first(self):
        for m, to in enumerate(SIDES):
            self.go((0, 0, m), (0, 0), (to, 0), 0, own=True)

    def pass_first(self):
        for m, to in enumerate(SIDES):
            self.got((0, 0, m), (-to, 0), 0)
            self.go((0, 1, m), (-to, 0), (to, 0), 1 + m)

    def second(self, b):
        along = self.ALONG[b]
        for m, to in enumerate(SIDES):
            if along == 2:
                self.got((0, 1, m), (along, 0), 1 + m)
        for m, to in enumerate(SIDES):
            self.go((1 + b, 0, m), (along, 0), (0, to), 0, own=not along)

    def pass_second(self, *bs):
        for b in bs:
            along = self.ALONG[b]
            for m, to in enumerate(SIDES):
                self.got((1 + b, 0, m), (along, -to), 0)
                self.go((1 + b, 1, m), (along, -to), (0, to), 1 + m)

    def end(self):
        for b, along in enumerate(self.ALONG):
            for m in BOTH:
                self.got((1 + b, 1, m), (along, 2), 1 + m)
        for c in self.sent: c.wait_send()


def _tail(*refs, axis, side, segs, parts, lr):
    wide, low, small, g1, gw1, *refs = refs
    (w_in, m_in, v_in), refs = sevens(refs)
    buf, gs_out, fac_out, *refs = refs
    (w_s, m_s, v_s), refs = sevens(refs)
    gs, new, sq_all, fac, wide_s, low_s, in_sem, g_sem, sq_send, sq_recv, ag_send, ag_recv, gs_sem, fac_sem, new_sem, *scr = refs
    third = len(scr) // 3
    group = side * side
    n = gs.shape[0]
    sq = Square(axis, side)
    me = sq.me
    unit = m_s[0].shape[1]

    sums = [pltpu.make_async_copy(a, gs.at[pl.ds(at, a.shape[0])], g_sem.at[i]) for i, (a, at) in enumerate(((g1, 0), (gw1, g1.shape[0])))]
    mine = [w.at[:, pl.ds(pl.multiple_of(me * m.shape[1], m.shape[1]), m.shape[1]), :] for w, m in zip(w_in, m_s)]
    loads = [pltpu.make_async_copy(a, b, in_sem.at[i]) for i, (a, b) in enumerate(zip((*mine, *m_in, *v_in), (*w_s, *m_s, *v_s)))]
    others = [lax.rem(me + d, group) for d in range(1, group)]
    for j in others:
        pl.semaphore_signal(pltpu.get_barrier_semaphore(), device_id={axis: j}, device_id_type=MESH)
    pl.semaphore_wait(pltpu.get_barrier_semaphore(), group - 1)

    early = g1.shape[0] + gw1.shape[0]
    big = second_rings(sq, wide, low, unit, pairs(scr[:third]))
    one = first_rings(sq, small, unit, pairs(scr[third:2 * third]))
    two = second_rings(sq, wide_s, low_s, unit, pairs(scr[2 * third:]))
    for r in one + big: r.start()
    for c in sums + loads: c.start()

    def squares(begin, end, total):
        def body(t, total):
            g = gs[pl.ds(pl.multiple_of(begin + t * unit, unit), unit), :].astype(F32)
            return total + (g * g).reshape(unit // 8, 8, LANES).sum(0)
        return lax.fori_loop(0, (end - begin) // unit, body, total)

    for r in one + big: r.middle()
    for c in sums: c.wait()
    total = squares(0, early, jnp.zeros(fac.shape, F32))
    for way, r in enumerate(one): r.finish(keeper(way, wide_s, low_s))
    for r in two: r.start()
    for way, r in enumerate(big): r.finish(rounder(way, gs, r.n, early))
    for r in two: r.middle()
    at = early + 2 * big[0].n
    total = squares(early, at, total)
    for way, r in enumerate(two): r.finish(rounder(way, gs, r.n, at))
    sq_all[0] = squares(at, n, total)
    swap = [pltpu.make_async_remote_copy(sq_all.at[0], sq_all.at[d], sq_send.at[d], sq_recv.at[d], device_id={axis: j}, device_id_type=MESH)
            for d, j in enumerate(others, 1)]
    for c in swap: c.start()
    for i, l, c, at, r in blocks_of(segs, 0, n):
        if r == LANES:
            gs[at:at + r, :] = gs[at:at + r, :].astype(F32).T.astype(BF)
    outs = gs_copy, fac_copy, new_copy = [pltpu.make_async_copy(*a) for a in ((gs, gs_out, gs_sem), (fac, fac_out, fac_sem), (new, buf.at[me], new_sem))]
    gs_copy.start()
    for c in loads: c.wait()
    for c in swap: c.wait_recv()
    mean = jnp.sum(sq_all[:].sum(0), keepdims=True) / float(n * LANES * group)
    fac[:] = jnp.broadcast_to(jnp.minimum(1.0, 0.5 * lax.rsqrt(mean + 1e-30)), fac.shape)
    fac_copy.start()

    starts = sorted(at for _, _, _, at, _ in blocks_of(segs, 0, n)) + [n]
    cuts = [min(starts, key=lambda r: abs(r - n * t // (2 * parts))) for t in range(2 * parts + 1)]
    spans = list(zip(cuts, cuts[1:]))
    gathers = []
    for c in range(parts):
        for h in BOTH:
            span = spans[h * parts + c]
            for i, l, cs, at, r in blocks_of(segs, *span):
                g = gs[at:at + r, :].astype(F32) * fac[0:1, :]
                m, v = moments(m_s[i][l, :, cs], v_s[i][l, :, cs], g)
                w = w_s[i][l, :, cs].astype(F32)
                new[at:at + r, :] = (w - lr * (m * lax.rsqrt(v + 1e-8) + 0.1 * w)).astype(BF)
            gathers.append(Gather(sq, h, c * 2 + h, span, new, buf, ag_send, ag_recv))
            gathers[-1].first()
    new_copy.start()
    near = 1, 2
    for c in range(parts):
        now, before = gathers[2 * c:2 * c + 2], gathers[max(2 * c - 2, 0):2 * c]
        for x in now: x.second(0)
        for x in now: x.pass_first()
        for x in now:
            for b in near: x.second(b)
        for x in before:
            x.second(3)
            x.pass_second(*near)
        for x in now: x.pass_second(0)
    for x in gathers[-2:]: x.second(3)
    for x in gathers[-2:]: x.pass_second(*near)
    for x in gathers: x.pass_second(3)
    for x in gathers: x.end()
    for c in swap: c.wait_send()
    for c in outs: c.wait()


def tail(wide, low, small, g1, gw1, weights, m, v, segs, n, axis, side, parts=3):
    k = len(m)
    group = side * side
    share = [a.shape for a in m]
    n_small = small.shape[2]
    unit = share[0][1]
    half = n_small // 2
    return pl.pallas_call(
        functools.partial(_tail, axis=axis, side=side, segs=segs, parts=parts, lr=0.02), name="tail",
        out_shape=[sd((group, n, LANES), BF), sd((n, LANES), BF), sd((8, LANES), F32)],
        in_specs=[any_] * (5 + 3 * k), out_specs=[any_] * 3,
        scratch_shapes=[vm(s, BF) for s in share] + [vm(s, F32) for s in share] * 2 +
                       [vm((n, LANES), BF), vm((n, LANES), BF), vm((group, 8, LANES), F32), vm((8, LANES), F32), vm((2, side, half, LANES), F32),
                        vm((2, side, half, LANES), BF), sem_of((3 * k,)), sem_of((2,)), sem_of((group,)), sem_of((group,)), *[sem_of((2 * parts, 5, 2, 2))] * 2, *[sem_of(())] * 3] +
                       ring_scratch(1, 2 * wide.shape[2], unit, F32) + ring_scratch(side, n_small, unit, BF) + ring_scratch(1, n_small, unit, F32),
        compiler_params=pltpu.CompilerParams(vmem_limit_bytes=FULL, **remote(4)),
    )(wide, low, small, g1, gw1, *weights, *m, *v)


def _finish(buf_ref, gs_ref, fac_ref, *refs, segs, k):
    (m_in, v_in, w_out), refs = sevens(refs)
    (m_out, v_out, m_s), refs = sevens(refs)
    v_s, (gs_s, g_sem, in_sem, out_sem) = refs[:k], refs[k:]
    i = pl.program_id(0)
    load_g = pltpu.make_async_copy(gs_ref, gs_s, g_sem)
    loads = [pltpu.make_async_copy(a, b, in_sem.at[n]) for n, (a, b) in enumerate(zip((*m_in, *v_in), (*m_s, *v_s)))]
    stores = [pltpu.make_async_copy(b, a, out_sem.at[n]) for n, (a, b) in enumerate(zip((*m_out, *v_out), (*m_s, *v_s)))]

    @on_first
    def _():
        for c in (load_g, *loads): c.start()

    for (a, l, rows, cols, at) in segs:
        for cb in range(cols // LANES):
            w_out[a][l, :, lanes(cb)] = buf_ref[at + cb * rows:at + cb * rows + rows, :]

    order = sorted(range(k), key=lambda a: -m_s[a].shape[2])
    for n, a in enumerate(order):
        @pl.when(i == 3 + n)
        def _(a=a, n=n):
            if n == 0: load_g.wait()
            loads[a].wait()
            loads[k + a].wait()
            fac = fac_ref[0:1, :]
            for (b, l, rows, cols, at) in segs:
                if b != a: continue
                for cb in range(cols // LANES):
                    g = gs_s[at + cb * rows:at + cb * rows + rows, :].astype(F32) * fac
                    here = (l, slice(None), lanes(cb))
                    m_s[a][here], v_s[a][here] = moments(m_s[a][here], v_s[a][here], g)
            stores[a].start()
            stores[k + a].start()

    @on_last
    def _():
        for c in stores: c.wait()


def finish(buf, gs, fac, weights, m, v, segs):
    group, n, _ = buf.shape
    k = len(m)
    share = [a.shape for a in m]
    return pl.pallas_call(
        functools.partial(_finish, segs=segs, k=k), name="finish", grid=(group,),
        in_specs=[pl.BlockSpec((None, n, LANES), lambda i: (i, 0, 0)), any_, whole(fac)] + [any_] * (2 * k),
        out_specs=[heads_block(*s) for s in share] + [any_] * (2 * k),
        out_shape=[sd(w.shape, BF) for w in weights] + [sd(s, F32) for s in share] * 2,
        scratch_shapes=[vm(s, F32) for s in share] * 2 + [vm((n, LANES), BF), sem_of(()), sem_of((2 * k,)), sem_of((2 * k,))],
        compiler_params=params(),
    )(buf, gs, fac, *m, *v)


def solution(mesh):
    axis = "dp"
    group = mesh.shape[axis]
    side = round(group**0.5)

    def step(x, dy, *arrays):
        weights, m, v = (arrays[i : i + 7] for i in (0, 7, 14))
        wq, wk, wv, wo, *mlp = weights
        h0, dy = x[0], dy[0]
        qkv = wq, wk, wv
        head = wk.shape[2]
        scale = head**-0.5
        unit = m[0].shape[1]
        cos, sin = tables(h0.shape[0], head, THETA)
        q0, k0, v0 = pre(h0, cos, sin, *qkv, 0)
        o0, lse0 = attend(q0, k0, v0, scale)
        h1, gate_up, h2, q1, k1, v1 = middle(o0, h0, cos, sin, wo, *mlp, *qkv, 0)
        o1, lse1 = attend(q1, k1, v1, scale)
        dh, do, delta, big, small1 = mlp_back(o1, h2, dy, wo, *mlp, 1, side, axis, bm=512)
        *d1, wide, low = attend_back(q1, k1, v1, do, lse1, delta, scale, big, side, axis, unit)
        dh, g1, small1 = pre_back(*d1, h2, cos, sin, 1, side, axis, small1, (dh, *qkv, wide, low))
        _, do, delta, big, small0, gw1 = mlp_back(o0, h1, dh, wo, *mlp, 0, side, axis, gate_up, small1)
        *d0, wide, low = attend_back(q0, k0, v0, do, lse0, delta, scale, big, side, axis, unit)
        (small0,) = pre_back(*d0, h0, cos, sin, 0, side, axis, small0)
        wq_, wk_, wv_, wo_, gate_, up_, down_ = range(7)
        order = [(i, l) for l in (1, 0) for i in (gate_, up_, down_, wo_, wq_, wk_, wv_)]
        segs, n = segments([w.shape for w in weights], order, group)
        buf, gs, fac = tail(wide, low, small0, g1, gw1, weights, m, v, segs, n, axis, side)
        return tuple(finish(buf, gs, fac, weights, m, v, segs))

    states, all_of, cut = P(("rep", "dp"), None, None), P(None, None, None), P(None, "dp", None)
    return jax.shard_map(
        step,
        mesh=mesh,
        in_specs=(states, states) + (all_of,) * 7 + (cut,) * 14,
        out_specs=(P("rep", None, None),) * 7 + (P("rep", "dp", None),) * 14,
        check_vma=False,
    )
```

```python
import functools

import jax
import jax.numpy as jnp
from jax import lax
from jax.experimental import pallas as pl
from jax.experimental.pallas import tpu as pltpu
from jax.sharding import PartitionSpec as P

BF, F32 = jnp.bfloat16, jnp.float32
THETA = 10000
LOG2E = 1.4426950408889634
HIDDEN = -1e30
BOTH = range(2)
SIDES = 1, -1


FULL = 63 * 2**20
LANES = 128


MESH = pl.DeviceIdType.MESH
sd, vm, sem_of = jax.ShapeDtypeStruct, pltpu.VMEM, pltpu.SemaphoreType.DMA
any_ = pl.BlockSpec(memory_space=pl.ANY)
in_vmem = pl.BlockSpec(memory_space=pltpu.VMEM)


def remote(n):
    return dict(collective_id=n, has_side_effects=True)


def params(held=(), spare=0, **more):
    room = FULL - spare - sum(a.size * a.dtype.itemsize for a in held)
    return pltpu.CompilerParams(dimension_semantics=("arbitrary",), vmem_limit_bytes=room, **more)


def stay(a):
    return pltpu.with_memory_space_constraint(a, vm)


def heads_block(heads, bm, d):
    return pl.BlockSpec((heads, bm, d), lambda i: (0, i, 0))


def stat_block(heads, bm):
    return pl.BlockSpec((heads, 1, bm), lambda i: (0, 0, i))


def on_first(run):
    pl.when(pl.program_id(0) == 0)(run)


def on_middle(run):
    pl.when(pl.program_id(0) == pl.num_programs(0) // 2)(run)


def on_last(run):
    pl.when(pl.program_id(0) == pl.num_programs(0) - 1)(run)


def iota(shape, axis):
    return lax.broadcasted_iota(jnp.int32, shape, axis)


def lanes(n, size=LANES):
    return slice(n * size, n * size + size)


def dot(a, b, ca=1, cb=0):
    return lax.dot_general(a, b, (((ca,), (cb,)), ((), ())), preferred_element_type=F32)

def mm(a, b):
    return dot(a, b).astype(BF)


def dot_nt(a, b):
    return dot(a, b, 1, 1)


def dot_tn(a, b):
    return dot(a, b, 0, 0)

def sigmoid(g):
    return 1.0 / (1.0 + jnp.exp(-g))


def mean(x):
    return jnp.mean(x, -1, keepdims=True)


def top_of(x):
    return x.max(0, keepdims=True)


def norm_of(h):
    wide = h.astype(F32)
    scale = lax.rsqrt(mean(wide * wide) + 1e-6)
    return wide, scale, (wide * scale).astype(BF)

def norm_back(db, wide, scale):
    return scale * db - wide * (scale * scale * scale * mean(db * wide))

def turn(t, cos, sin):
    return t * cos + pltpu.roll(t, t.shape[1] // 2, 1) * sin

def tables(tokens, head, theta):
    half = head // 2
    rate = theta ** (-jnp.arange(half, dtype=F32) / half)
    low = 64
    a = (jnp.arange(tokens // low, dtype=F32) * low)[:, None] * rate
    b = jnp.arange(low, dtype=F32)[:, None] * rate
    ca, sa, cb, sb = (f(t) for t in (a, b) for f in (jnp.cos, jnp.sin))
    ca, sa, cb, sb = ca[:, None], sa[:, None], cb[None], sb[None]
    cos, sin = (ca * cb - sa * sb).reshape(tokens, half), (sa * cb + ca * sb).reshape(tokens, half)
    return jnp.concatenate([cos, cos], 1), jnp.concatenate([-sin, sin], 1)

def whole(a, layer=None):
    one = layer is not None
    return pl.BlockSpec((None,) * one + a.shape[one:], lambda *_: (layer,) * one + (0,) * (a.ndim - one), pipeline_mode=pl.Buffered(1))

def rows(bm, width):
    return pl.BlockSpec((bm, width), lambda i: (i, 0))

def heads_of(ref):
    return jnp.concatenate([ref[n] for n in range(ref.shape[0])], axis=1)

def project(a, wq, wk, wv, cos, sin, q_ref, k_ref, v_ref):
    hd = cos.shape[1]
    q = mm(a, wq).astype(F32)
    for n in range(q.shape[1] // hd):
        q_ref[n] = turn(q[:, lanes(n, hd)], cos, sin).astype(BF)
    k_ref[:] = turn(mm(a, wk).astype(F32), cos, sin).astype(BF)
    v_ref[:] = mm(a, wv)

def _pre(h_ref, cos_ref, sin_ref, wq, wk, wv, q_ref, k_ref, v_ref):
    _, _, a = norm_of(h_ref[:])
    project(a, wq[:], wk[:], wv[:], cos_ref[:], sin_ref[:], q_ref, k_ref, v_ref)

def pre(h, cos, sin, wq, wk, wv, layer, bm=512):
    t, d = h.shape
    hd = cos.shape[1]
    nh = wq.shape[2] // hd
    return pl.pallas_call(
        _pre, name="pre", grid=(t // bm,),
        in_specs=[rows(bm, d), rows(bm, hd), rows(bm, hd), whole(wq, layer), whole(wk, layer), whole(wv, layer)],
        out_specs=[heads_block(nh, bm, hd), rows(bm, hd), rows(bm, hd)],
        out_shape=[sd((nh, t, hd), BF), sd((t, hd), BF), sd((t, hd), BF)],
        compiler_params=params(),
    )(h, cos, sin, wq, wk, wv)

def fetch(pairs, sem):
    return [pltpu.make_async_copy(a, b, sem.at[n]) for n, (a, b) in enumerate(pairs)]

def _mid(o_ref, h_ref, cos_ref, sin_ref, wo, wg, wu, wd, wq, wk, wv, h1_ref, gu_ref, h2_ref, q_ref, k_ref, v_ref,
         wo_s, wg_s, wu_s, wd_s, wq_s, wk_s, wv_s, sem, *, layer, part):
    i = pl.program_id(0)
    cps = fetch([(a.at[layer], b) for a, b in ((wo, wo_s), (wg, wg_s), (wu, wu_s), (wd, wd_s))] +
                [(a.at[layer + 1], b) for a, b in ((wq, wq_s), (wk, wk_s), (wv, wv_s))], sem)

    @on_first
    def _():
        for c in cps: c.start()
        cps[0].wait()

    h1 = h_ref[:] + mm(heads_of(o_ref), wo_s[:])
    h1_ref[:] = h1
    _, _, b = norm_of(h1)

    @on_first
    def _():
        for c in cps[1:]: c.wait()

    f = wg_s.shape[1]
    y = None
    for at in range(0, f, part):
        c = slice(at, at + part)
        g, u = dot(b, wg_s[:, c]), dot(b, wu_s[:, c])
        gu_ref[:, c] = g
        gu_ref[:, f + at:f + at + part] = u
        act = (g * sigmoid(g) * u).astype(BF)
        yc = dot(act, wd_s[c, :])
        y = yc if y is None else y + yc
    h2 = h1 + y.astype(BF)
    h2_ref[:] = h2
    _, _, a = norm_of(h2)
    project(a, wq_s[:], wk_s[:], wv_s[:], cos_ref[:], sin_ref[:], q_ref, k_ref, v_ref)

def middle(o, h, cos, sin, wo, wg, wu, wd, wq, wk, wv, layer, bm=512, part=512):
    t, d = h.shape
    nh, _, hd = o.shape
    f = wg.shape[2]
    hs = heads_block(nh, bm, hd)
    return pl.pallas_call(
        functools.partial(_mid, layer=layer, part=part), name="middle", grid=(t // bm,),
        in_specs=[hs, rows(bm, d), rows(bm, hd), rows(bm, hd)] + [any_] * 7,
        out_specs=[rows(bm, d), rows(bm, 2 * f), rows(bm, d), hs, rows(bm, hd), rows(bm, hd)],
        out_shape=[sd((t, d), BF), sd((t, 2 * f), F32), sd((t, d), BF), sd((nh, t, hd), BF), sd((t, hd), BF), sd((t, hd), BF)],
        scratch_shapes=[vm(w.shape[1:], BF) for w in (wo, wg, wu, wd, wq, wk, wv)] + [sem_of((7,))],
        compiler_params=params(),
    )(o, h, cos, sin, wo, wg, wu, wd, wq, wk, wv)


class Square:
    def __init__(self, axis, side):
        self.axis, self.side = axis, side
        me = lax.axis_index(axis)
        self.me = me
        self.place = lax.div(me, side), lax.rem(me, side)

    def at(self, way, along, across=0):
        x, y = (lax.rem(p + (along if n == way else across) + self.side, self.side) for n, p in enumerate(self.place))
        return x * self.side + y

    def greet(self):
        for way in BOTH:
            for step in SIDES:
                pl.semaphore_signal(pltpu.get_barrier_semaphore(), device_id={self.axis: self.at(way, step)}, device_id_type=MESH)

    def met(self):
        pl.semaphore_wait(pltpu.get_barrier_semaphore(), 4)


class Ring:
    KINDS = "far", "free", "joined"

    def __init__(self, sq, way, send, keep, n, unit, s):
        self.sq, self.way, self.send, self.keep, self.unit = sq, way, send, keep, unit
        self.first, self.final, self.mid, self.own, self.out, self.send_sem, self.recv_sem, self.sem, self.own_sem = s
        cut = n // unit // 2 * unit
        self.halves = (0, cut), (cut, n - cut)
        self.n = n

    @staticmethod
    def scratch(k, n, unit, kept):
        most = n - n // unit // 2 * unit
        part, full = (len(BOTH), k, most, LANES), (k, n, LANES)
        return [vm(part, BF), vm((len(BOTH), *full), BF), vm(part, kept), vm(full, kept), vm(part, BF)] + [sem_of((3, len(BOTH)))] * 2 + [sem_of((len(BOTH),)), sem_of(())]

    def block(self, step):
        return lax.rem(self.sq.place[self.way] + step + self.sq.side, self.sq.side)

    def copy(self, kind, d):
        half = 1 - d if kind == "free" else d
        rows, size = pl.ds(*self.halves[half]), pl.ds(0, self.halves[half][1])
        src = self.out.at[d, :, size] if kind == "joined" else self.send(self.block(2 if kind == "far" else SIDES[d]), rows)
        dst = self.first.at[d, :, size] if kind == "far" else self.final.at[d, :, rows]
        n = self.KINDS.index(kind), d
        to = {self.sq.axis: self.sq.at(self.way, SIDES[d])}
        return pltpu.make_async_remote_copy(src, dst, self.send_sem.at[n], self.recv_sem.at[n], device_id=to, device_id_type=MESH)

    def added(self, d):
        rows, size = pl.ds(*self.halves[d]), self.halves[d][1]
        return pltpu.make_async_copy(self.keep(self.block(SIDES[d]), rows), self.mid.at[d, :, pl.ds(0, size)], self.sem.at[d])

    def mine(self):
        return pltpu.make_async_copy(self.keep(self.block(0), pl.ds(0, self.n)), self.own, self.own_sem)

    def start(self):
        for kind in self.KINDS[:2]:
            for d in BOTH:
                self.copy(kind, d).start()
        for d in BOTH:
            self.added(d).start()
        self.mine().start()

    def steps(self, size, run):
        def body(t, _):
            run(pl.ds(pl.multiple_of(t * self.unit, self.unit), self.unit))
            return _

        lax.fori_loop(0, size // self.unit, body, 0)

    def middle(self):
        for d in BOTH:
            self.copy("far", d).wait_recv()
            self.added(d).wait()

            def add(here, d=d):
                self.out[d, :, here] = (self.mid[d, :, here].astype(F32) + self.first[d, :, here].astype(F32)).astype(BF)

            self.steps(self.halves[d][1], add)
            self.copy("joined", d).start()

    def finish(self, put):
        for d in BOTH:
            for kind in self.KINDS[1:]:
                self.copy(kind, d).wait_recv()
        self.mine().wait()
        self.steps(self.n, lambda here: put(here, self.own[:, here].astype(F32) + sum(self.final[d, :, here].astype(F32) for d in BOTH)))
        for d in BOTH:
            for kind in self.KINDS:
                self.copy(kind, d).wait_send()


def first_rings(sq, g, unit, scr):
    n = g.shape[2] // 2
    x_block = lambda p, rows: g.at[p, :, rows]
    y_block = lambda p, rows: g.at[:, p, pl.ds(rows.start + n, rows.size)]
    return [Ring(sq, way, block, block, n, unit, scr[way]) for way, block in enumerate((x_block, y_block))]


def second_rings(sq, wide, low, unit, scr):
    pick = lambda ref, way: (lambda p, rows: ref.at[way, pl.ds(p, 1), rows])
    return [Ring(sq, 1 - way, pick(low, way), pick(wide, way), wide.shape[2], unit, scr[way]) for way in BOTH]


def ring_scratch(k, n, unit, kept):
    return Ring.scratch(k, n // 2, unit, kept) * 2


def pairs(scr):
    half = len(scr) // 2
    return scr[:half], scr[half:]


def keeper(way, wide, low):
    def put(rows, total):
        wide[way, :, rows] = total
        low[way, :, rows] = total.astype(BF)
    return put


def rounder(way, g, n, at=0):
    def put(rows, total):
        g[pl.ds(pl.multiple_of(rows.start + (at + way * n), 16), rows.size)] = total[0].astype(BF)
    return put


def leave(sq, way, ring, low, wide, sem):
    q, side = sq.place[1 - way], sq.side
    full, (one, other) = pl.ds(0, ring.n), (pl.ds(*h) for h in ring.halves)
    got = []
    for pair, parts in ((wide, (full, one, None, other)), (low, (None, other, full, one))):
        for step, part in enumerate(parts):
            if part:
                at = way, lax.rem(q + step, side), part
                got.append(pltpu.make_async_copy(pair[0].at[at], pair[1].at[at], sem.at[len(got)]))
                got[-1].start()
    return got


def _attend(q_ref, k_ref, v_ref, o_ref, lse_ref, s_a, s_b, top_a, top_b, vt_s, gap_s, *, scale, bq):
    heads, _, d = q_ref.shape
    tokens = k_ref.shape[0]
    iq = pl.program_id(0)
    e = scale * LOG2E

    @on_first
    def _():
        vt_s[:d, :] = v_ref[:].astype(F32).T.astype(BF)
        vt_s[d:, :] = jnp.ones_like(vt_s[d:, :])
        gap_s[:] = iota(gap_s.shape, 1) - iota(gap_s.shape, 0)

    half = bq // 2

    def score(n, keys, s_ref, top_ref):
        q = q_ref[n]
        cut = keys - half
        top = None
        if keys > bq:
            s = dot_nt(k_ref[:keys - bq, :], q)
            s_ref[:keys - bq, :] = s
            top = top_of(s)
        near = dot_nt(k_ref[keys - bq:cut, :], q)
        left = jnp.where(gap_s[:] >= 0, near[:, :half], HIDDEN)
        right = near[:, half:]
        s_ref[keys - bq:cut, :half] = left
        s_ref[keys - bq:cut, half:] = right
        far = jnp.where(gap_s[:] >= 0, dot_nt(k_ref[cut:keys, :], q[half:, :]), HIDDEN)
        s_ref[cut:keys, half:] = far
        m = jnp.concatenate([top_of(left), jnp.maximum(top_of(right), top_of(far))], 1)
        top_ref[:] = m if top is None else jnp.maximum(m, top)

    def weigh(n, keys, s_ref, top_ref):
        cut = keys - half
        top = top_ref[:]
        pa = jnp.exp2((s_ref[:cut, :] - top) * e).astype(BF)
        pb = jnp.exp2((s_ref[cut:keys, half:] - top[:, half:]) * e).astype(BF)
        mix = dot(vt_s[:, :cut], pa)
        more = dot(vt_s[:, cut:keys], pb)
        mix = jnp.concatenate([mix[:, :half], mix[:, half:] + more], 1)
        total = mix[d:d + 1, :]
        o_ref[n] = (mix[:d, :] * (1.0 / total)).T.astype(o_ref.dtype)
        lse_ref[n] = top * scale + jnp.log(total)

    for j in range(tokens // bq):
        @pl.when(iq == j)
        def _(keys=(j + 1) * bq):
            score(0, keys, s_a, top_a)

            def pair(t, _):
                score(2 * t + 1, keys, s_b, top_b)
                weigh(2 * t, keys, s_a, top_a)
                score(2 * t + 2, keys, s_a, top_a)
                weigh(2 * t + 1, keys, s_b, top_b)
                return _

            lax.fori_loop(0, heads // 2 - 1, pair, 0)
            score(heads - 1, keys, s_b, top_b)
            weigh(heads - 2, keys, s_a, top_a)
            weigh(heads - 1, keys, s_b, top_b)

def attend(q, k, v, scale, bq=512):
    heads, tokens, d = q.shape
    here = heads_block(heads, bq, d)
    all_ = whole(k)
    return pl.pallas_call(
        functools.partial(_attend, scale=scale, bq=bq), name="attend", grid=(tokens // bq,),
        in_specs=[here, all_, all_],
        out_specs=[here, stat_block(heads, bq)],
        out_shape=[sd(q.shape, BF), sd((heads, 1, tokens), F32)],
        scratch_shapes=[vm((tokens, bq), F32), vm((tokens, bq), F32), vm((1, bq), F32), vm((1, bq), F32),
                        vm((d + 8, tokens), BF), vm((bq // 2, bq // 2), jnp.int32)],
        compiler_params=params(),
    )(q, k, v)
def _attend_back(q_ref, k_ref, v_ref, do_ref, lse_ref, delta_ref, g_ref, dq_ref, dk_ref, dv_ref, wide_ref, low_ref,
                 s_a, s_b, dp_a, dp_b, kt_s, vt_s, dkt_s, dvt_s, gap_s, wide_s, low_s, sem, *scr, scale, bq, side, axis, unit):
    heads, _, d = q_ref.shape
    tokens = k_ref.shape[0]
    iq = pl.program_id(0)
    e = scale * LOG2E
    half = bq // 2

    sq = Square(axis, side)
    rings = first_rings(sq, g_ref, unit, pairs(scr))
    last = pl.num_programs(0) - 1

    @on_first
    def _():
        sq.greet()
        row = iota((d, tokens), 0)
        kt_s[:d, :] = k_ref[:].astype(F32).T.astype(BF)
        kt_s[d:, :] = jnp.where(row < 3, 1.0, 0.0).astype(BF)
        vt_s[:d, :] = v_ref[:].astype(F32).T.astype(BF)
        vt_s[d:, :] = jnp.where((row >= 3) & (row < 6), 1.0, 0.0).astype(BF)
        gap_s[:] = iota(gap_s.shape, 0) - iota(gap_s.shape, 1)
        dkt_s[:] = jnp.zeros_like(dkt_s)
        dvt_s[:] = jnp.zeros_like(dvt_s)
        sq.met()
        for r in rings: r.start()

    @on_last
    def _():
        for r in rings: r.middle()

    def parts(x):
        a = x.astype(BF).astype(F32)
        b = (x - a).astype(BF).astype(F32)
        return [a, b, x - a - b]

    def score(n, keys, s_ref, dp_ref):
        cut = keys - half
        row = iota((d, bq), 0)
        rows = jnp.zeros((d, bq), F32)
        for i, x in enumerate(parts(lse_ref[n] * (-1 / scale)) + parts(-delta_ref[n])):
            rows = jnp.where(row == i, x, rows)
        extra = rows.T.astype(BF)
        q = jnp.concatenate([q_ref[n], extra], 1)
        do = jnp.concatenate([do_ref[n], extra], 1)
        if keys > bq:
            s_ref[:, :keys - bq] = dot(q, kt_s[:, :keys - bq])
        near = dot(q, kt_s[:, keys - bq:cut])
        s_ref[:half, keys - bq:cut] = jnp.where(gap_s[:] >= 0, near[:half], HIDDEN)
        s_ref[half:, keys - bq:cut] = near[half:]
        s_ref[half:, cut:keys] = jnp.where(gap_s[:] >= 0, dot(q[half:], kt_s[:, cut:keys]), HIDDEN)
        dp_ref[:, :cut] = dot(do, vt_s[:, :cut])
        dp_ref[half:, cut:keys] = dot(do[half:], vt_s[:, cut:keys])

    def weigh(n, keys, s_ref, dp_ref):
        cut = keys - half
        qt = q_ref[n].astype(F32).T.astype(BF)
        dot_ = do_ref[n].astype(F32).T.astype(BF)
        pa = jnp.exp2(s_ref[:, :cut] * e)
        da = (pa * dp_ref[:, :cut]).astype(BF)
        pb = jnp.exp2(s_ref[half:, cut:keys] * e)
        db = (pb * dp_ref[half:, cut:keys]).astype(BF)
        dvt_s[:, :cut] += dot(dot_, pa.astype(BF))
        dkt_s[:, :cut] += dot(qt, da)
        dvt_s[:, cut:keys] += dot(dot_[:, half:], pb.astype(BF))
        dkt_s[:, cut:keys] += dot(qt[:, half:], db)
        dq = dot(da, k_ref[:cut, :])
        far = dot(db, k_ref[cut:keys, :])
        dq_ref[n, :half] = (dq[:half] * scale).astype(BF)
        dq_ref[n, half:] = ((dq[half:] + far) * scale).astype(BF)

    for j in range(tokens // bq):
        @pl.when(iq == j)
        def _(keys=(j + 1) * bq):
            score(0, keys, s_a, dp_a)

            def pair(t, _):
                score(2 * t + 1, keys, s_b, dp_b)
                weigh(2 * t, keys, s_a, dp_a)
                score(jnp.minimum(2 * t + 2, heads - 1), keys, s_a, dp_a)
                weigh(2 * t + 1, keys, s_b, dp_b)
                return _

            lax.fori_loop(0, heads // 2, pair, 0)

    @on_last
    def _():
        outs = []
        for way, r in enumerate(rings):
            r.finish(keeper(way, wide_s, low_s))
            outs += leave(sq, way, r, (low_s, low_ref), (wide_s, wide_ref), sem.at[way])
        dk_ref[:] = (dkt_s[:] * scale).T.astype(BF)
        dv_ref[:] = dvt_s[:].T.astype(BF)
        for c in outs: c.wait()

def attend_back(q, k, v, do, lse, delta, scale, g, side, axis, unit, bq=512):
    n = g.shape[2]
    half = (2, side, n // 2, LANES)
    heads, tokens, d = q.shape
    here = heads_block(heads, bq, d)
    all_ = whole(k)
    stat = stat_block(heads, bq)
    return pl.pallas_call(
        functools.partial(_attend_back, scale=scale, bq=bq, side=side, axis=axis, unit=unit), name="attend_back", grid=(tokens // bq,),
        in_specs=[here, all_, all_, here, stat, stat, any_],
        out_specs=[here, all_, all_, any_, any_],
        out_shape=[sd(q.shape, BF)] + [sd(k.shape, BF)] * 2 + [sd(half, F32), sd(half, BF)],
        scratch_shapes=[vm((bq, tokens), F32)] * 4 + [vm((2 * d, tokens), BF)] * 2 + [vm((d, tokens), F32)] * 2 +
                       [vm((bq // 2, bq // 2), jnp.int32), vm(half, F32), vm(half, BF), sem_of((2, 6))] + ring_scratch(side, n, unit, BF),
        compiler_params=params(**remote(1)),
    )(q, k, v, do, lse, delta, g)


def split_rows(x, side, r):
    return x.astype(BF).reshape(side, side, r, x.shape[1])


def put_columns(acc, stage, at, side):
    r = acc.shape[0] // (side * side)
    for cb in range(acc.shape[1] // LANES):
        stage[:, :, at:at + r, :] = split_rows(acc[:, lanes(cb)], side, r)
        at += r
    return at


def sync(a, b, sem):
    c = pltpu.make_async_copy(a, b, sem.at[0])
    c.start()
    c.wait()


def copy_rows(stage, out, at, sem):
    c = pltpu.make_async_copy(stage, out.at[:, :, pl.ds(at, stage.shape[2])], sem)
    c.start()
    return c


def mlp_body(i, o, h1, dy, gu, w, acc, dh_ref, do_ref, delta_ref, part):
    wo_s, wg_s, wu_s, wd_s = w
    dwg_s, dwu_s, dwd_s, dwo_s = acc
    heads, _, hd = do_ref.shape
    wide, scale, b = norm_of(h1)
    db = None
    for at in range(0, wg_s.shape[1], part):
        c = slice(at, at + part)
        g, u = gu(c) if gu else (dot(b, wg_s[:, c]), dot(b, wu_s[:, c]))
        da = dot_nt(dy, wd_s[c, :]).astype(BF).astype(F32)
        s = sigmoid(g)
        silu = g * s
        act = (silu * u).astype(BF)
        du = (da * silu).astype(BF)
        dg = (da * u * (s + silu * (1.0 - s))).astype(BF)
        dbc = dot_nt(dg, wg_s[:, c]) + dot_nt(du, wu_s[:, c])
        db = dbc if db is None else db + dbc
        dwg_s[:, c] += dot_tn(b, dg)
        dwu_s[:, c] += dot_tn(b, du)
        dwd_s[:, c] += dot_tn(dy, act)
    dh = dy + norm_back(db.astype(BF).astype(F32), wide, scale).astype(BF)
    dh_ref[:] = dh
    do = dot_nt(dh, wo_s[:]).astype(BF)
    prod = do.astype(F32) * o.astype(F32)
    lane = iota((dy.shape[0], LANES), 1)
    table = jnp.zeros((dy.shape[0], LANES), F32)
    for n in range(heads):
        c = lanes(n, hd)
        do_ref[n] = do[:, c]
        table = jnp.where(lane == n, jnp.sum(prod[:, c], -1, keepdims=True), table)
    table = table.T
    for n in range(heads):
        delta_ref[n] = table[n:n + 1, :]
    dwo_s[:] += dot_tn(o, dh)


def _mlp_back(*refs, layer, part, side, axis, kept):
    i, steps = pl.program_id(0), pl.num_programs(0)
    o_ref, h_ref, dy_ref, *refs = refs
    if kept:
        gu_ref, *refs = refs
    wo, wg, wu, wd, *refs = refs
    if kept:
        early, *refs = refs
    dh_ref, do_ref, delta_ref, big, small, *refs = refs
    if kept:
        g_out, *refs = refs
    wo_s, wg_s, wu_s, wd_s, dwg_s, dwu_s, dwd_s, dwo_s, st_a, st_b, sem, sem_a, sem_b, *refs = refs
    w, acc = (wo_s, wg_s, wu_s, wd_s), (dwg_s, dwu_s, dwd_s, dwo_s)
    cps = [pltpu.make_async_copy(a.at[layer], b, sem.at[n]) for n, (a, b) in enumerate(zip((wo, wg, wu, wd), w))]
    if kept:
        wide_s, low_s, g_s, *scr = refs
        sq = Square(axis, side)
        unit = dh_ref.shape[1] // (side * side)
        half = len(scr) // 2
        one = first_rings(sq, early, unit, pairs(scr[:half]))
        two = second_rings(sq, wide_s, low_s, unit, pairs(scr[half:]))

    @on_first
    def _():
        for c in cps: c.start()
        if kept: sq.greet()
        for r in acc: r[:] = jnp.zeros_like(r)
        if kept:
            sq.met()
            for r in one: r.start()
        for c in cps: c.wait()

    if kept:
        @pl.when(i == steps // 2 - 1)
        def _():
            for r in one: r.middle()

        @pl.when(i == steps // 2 + 1)
        def _():
            for way, r in enumerate(one): r.finish(keeper(way, wide_s, low_s))
            for r in two: r.start()

        @on_last
        def _():
            for r in two: r.middle()

    o, dy = heads_of(o_ref), dy_ref[:]
    if kept:
        f = gu_ref.shape[1] // 2
        mlp_body(i, o, h_ref[:], dy, lambda c: (gu_ref[:, c], gu_ref[:, c.start + f:c.stop + f]), w, acc, dh_ref, do_ref, delta_ref, part)
    else:
        mlp_body(i, o, h_ref[:] + mm(o, wo_s[:]), dy, None, w, acc, dh_ref, do_ref, delta_ref, part)

    @on_last
    def _():
        n = st_a.shape[2]
        put_columns(dwg_s, st_a, 0, side)
        first = copy_rows(st_a, big, 0, sem_a)
        put_columns(dwu_s, st_b, 0, side)
        second = copy_rows(st_b, big, n, sem_b)
        first.wait()
        for x in range(side):
            for y in range(side):
                st_a[x, y] = dwd_s[:, lanes(x * side + y)].astype(BF)
        third = copy_rows(st_a, big, 2 * n, sem_a)
        second.wait()
        size = put_columns(dwo_s, st_b, 0, side)
        fourth = copy_rows(st_b.at[:, :, pl.ds(0, size)], small, 0, sem_b)
        if kept:
            for way, r in enumerate(two): r.finish(rounder(way, g_s, r.n))
            sync(g_s, g_out, sem)
        third.wait()
        fourth.wait()


def mlp_back(o, h, dy, wo, wg, wu, wd, layer, side, axis, gu=None, early=None, bm=256, part=512):
    t, d = h.shape
    nh, _, hd = o.shape
    f = wg.shape[2]
    kept = gu is not None
    hs = heads_block(nh, bm, hd)
    unit = d // (side * side)
    n_wo = d // LANES * unit
    n_own = n_wo if kept else n_wo + (nh + 2) * unit
    n_small = early.shape[2] if kept else 0
    given = [o, h, dy] + [gu] * kept + [wo, wg, wu, wd] + [early] * kept
    half = n_small // 2
    return pl.pallas_call(
        functools.partial(_mlp_back, layer=layer, part=part, side=side, axis=axis, kept=kept), name=f"mlp_back{layer}", grid=(t // bm,),
        in_specs=[hs, rows(bm, d), rows(bm, d)] + [rows(bm, 2 * f)] * kept + [any_] * (4 + kept),
        out_specs=[rows(bm, d), hs, stat_block(nh, bm)] + [any_] * (2 + kept),
        out_shape=[sd((t, d), BF), sd((nh, t, hd), BF), sd((nh, 1, t), F32), sd((side, side, 3 * d, LANES), BF), sd((side, side, n_own, LANES), BF)] +
                  [sd((n_small, LANES), BF)] * kept,
        scratch_shapes=[vm(w.shape[1:], BF) for w in (wo, wg, wu, wd)] + [vm((d, f), F32)] * 3 + [vm((d, d), F32)] + [vm((side, side, d, LANES), BF)] * 2 +
                       [sem_of((4,)), sem_of(()), sem_of(())] +
                       ([vm((2, side, half, LANES), F32), vm((2, side, half, LANES), BF), vm((n_small, LANES), BF)] +
                        ring_scratch(side, n_small, unit, BF) + ring_scratch(1, n_small, unit, F32) if kept else []),
        compiler_params=params(**(remote(3) if kept else {})),
    )(*given)


def project_back(dq_ref, dk_ref, dv_ref, h_ref, cos_ref, sin_ref, dw_s):
    cos, sin = cos_ref[:], -sin_ref[:]
    wide, scale, a = norm_of(h_ref[:])
    dk = turn(dk_ref[:].astype(F32), cos, sin).astype(BF)
    dq = jnp.concatenate([turn(dq_ref[n].astype(F32), cos, sin).astype(BF) for n in range(dq_ref.shape[0])], 1)
    ds = dq, dk, dv_ref[:]
    dw_s[:] += dot_tn(a, jnp.concatenate(ds, 1))
    return wide, scale, ds


def _pre_back(dq_ref, dk_ref, dv_ref, h_ref, cos_ref, sin_ref, wide, low, dh_ref, wq, wk, wv, _, out_dh, g_out, out, dw_s, stage,
              out_sem, sem, g_s, *scr, side, axis):
    sq = Square(axis, side)
    rings = second_rings(sq, wide, low, h_ref.shape[1] // (side * side), pairs(scr))

    @on_first
    def _():
        sq.greet()
        dw_s[:] = jnp.zeros_like(dw_s)
        sq.met()
        for r in rings: r.start()

    @on_middle
    def _():
        for r in rings: r.middle()

    wide_h, scale, ds = project_back(dq_ref, dk_ref, dv_ref, h_ref, cos_ref, sin_ref, dw_s)
    da = sum(dot_nt(d, w[:]) for d, w in zip(ds, (wq, wk, wv)))
    out_dh[:] = dh_ref[:] + norm_back(da.astype(BF).astype(F32), wide_h, scale).astype(BF)

    @on_last
    def _():
        put_columns(dw_s, stage, 0, side)
        c = copy_rows(stage, out, out.shape[2] - stage.shape[2], out_sem)
        for way, r in enumerate(rings): r.finish(rounder(way, g_s, r.n))
        sync(g_s, g_out, sem)
        c.wait()


def pre_back_specs(nh, hd, d, bm):
    return [heads_block(nh, bm, hd), rows(bm, hd), rows(bm, hd), rows(bm, d), rows(bm, hd), rows(bm, hd), any_, any_]


def pre_back(dq, dk, dv, wide, low, h, cos, sin, layer, side, axis, small, dh, *ws, bm=512):
    t, d = h.shape
    nh, _, hd = dq.shape
    unit = d // (side * side)
    packed = side, side, (nh + 2) * unit, LANES
    n = wide.shape[2] * len(BOTH)
    return pl.pallas_call(
        functools.partial(_pre_back, side=side, axis=axis), name="pre_back", grid=(t // bm,),
        in_specs=pre_back_specs(nh, hd, d, bm) + [rows(bm, d)] + [whole(w, layer) for w in ws] + [any_],
        out_specs=[rows(bm, d)] + [any_] * 2,
        out_shape=[sd((t, d), BF), sd((n, LANES), BF), sd(small.shape, BF)],
        input_output_aliases={9 + len(ws): 2},
        scratch_shapes=[vm((d, (nh + 2) * hd), F32), vm(packed, BF), sem_of(()), sem_of((1,)), vm((n, LANES), BF)] + ring_scratch(1, n, unit, F32),
        compiler_params=params(**remote(2)),
    )(dq, dk, dv, h, cos, sin, wide, low, dh, *ws, small)


def segments(shapes, order, group):
    out, at = [], 0
    for i, l in order:
        r, c = shapes[i][1] // group, shapes[i][2]
        out.append((i, l, r, c, at))
        at += r * c // LANES
    return out, at


def moments(m, v, g):
    return 0.9 * m + 0.1 * g, 0.95 * v + 0.05 * g * g


def blocks_of(segs, begin, end):
    for i, l, r, c, at in segs:
        for cb in range(c // LANES):
            if begin <= at + cb * r < end:
                yield i, l, lanes(cb), at + cb * r, r


def sevens(refs, k=7):
    return [refs[i * k:i * k + k] for i in range(3)], refs[3 * k:]


class Gather:
    ALONG = 0, -1, 1, 2

    def __init__(self, sq, way, part, span, new, buf, send_sem, recv_sem):
        self.sq, self.way, self.part, self.new, self.buf, self.sems, self.sent = sq, way, part, new, buf, (send_sem, recv_sem), []
        begin, end = span
        mid = begin + (end - begin) // 32 * 16
        self.spans = (begin, end - begin), (begin, mid - begin), (mid, end - mid)

    def copy(self, m, source, to, which):
        along, across = source
        owner = self.sq.at(self.way, along, across)
        rows = pl.ds(*self.spans[which])
        place = self.buf.at[owner, rows]
        s, r = (x.at[self.part, *m] for x in self.sems)
        mine = source == (0, 0)
        return pltpu.make_async_remote_copy(self.new.at[rows] if mine else place, place, s, r, device_id={self.sq.axis: self.sq.at(self.way, *to)}, device_id_type=MESH)

    def go(self, *a, **k):
        c = self.copy(*a, **k)
        c.start()
        self.sent.append(c)

    def got(self, m, source, which):
        self.copy(m, source, (1, 0), which).wait_recv()

    def first(self):
        for m, to in enumerate(SIDES):
            self.go((0, 0, m), (0, 0), (to, 0), 0)

    def pass_first(self):
        for m, to in enumerate(SIDES):
            self.got((0, 0, m), (-to, 0), 0)
            self.go((0, 1, m), (-to, 0), (to, 0), 1 + m)

    def second(self, b):
        along = self.ALONG[b]
        for m, to in enumerate(SIDES):
            if along == 2:
                self.got((0, 1, m), (along, 0), 1 + m)
        for m, to in enumerate(SIDES):
            self.go((1 + b, 0, m), (along, 0), (0, to), 0)

    def pass_second(self, *bs):
        for b in bs:
            along = self.ALONG[b]
            for m, to in enumerate(SIDES):
                self.got((1 + b, 0, m), (along, -to), 0)
                self.go((1 + b, 1, m), (along, -to), (0, to), 1 + m)

    def end(self):
        for b, along in enumerate(self.ALONG):
            for m in BOTH:
                self.got((1 + b, 1, m), (along, 2), 1 + m)
        for c in self.sent: c.wait_send()


def _tail(*refs, axis, side, segs, parts, lr):
    *token_refs, wide, low, g1, gw1, wo_ref = refs[:11]
    (w_in, m_in, v_in), refs = sevens(refs[11:])
    buf, *refs = refs
    (m_s, v_s, w_s), refs = sevens(refs)
    dw_s, small, gs, new, own_sem, sq_all, fac, wide_w, low_w, wide_s, low_s, in_sem, g_sem, sq_send, sq_recv, ag_send, ag_recv, *scr = refs
    part = len(scr) // 5
    ring_s = [pairs(scr[i:i + part]) for i in range(0, len(scr), part)]
    group = side * side
    n = gs.shape[0]
    sq = Square(axis, side)
    me = sq.me
    unit = m_s[0].shape[1]
    early = g1.shape[0] + gw1.shape[0]
    late = n - small.shape[2]
    big, wo_two, two = (second_rings(sq, a, b, unit, r) for a, b, r in zip((wide, wide_w, wide_s), (low, low_w, low_s), ring_s))
    wo_one, one = (first_rings(sq, a, unit, r) for a, r in zip((wo_ref, small), ring_s[3:]))
    wo_at = late - wo_ref.shape[2]
    sums = [pltpu.make_async_copy(a, gs.at[pl.ds(at, a.shape[0])], g_sem.at[i]) for i, (a, at) in enumerate(((g1, 0), (gw1, g1.shape[0])))]
    mine = [w.at[:, pl.ds(pl.multiple_of(me * m.shape[1], m.shape[1]), m.shape[1]), :] for w, m in zip(w_in, m_s)]
    loads = [pltpu.make_async_copy(a, b, in_sem.at[i]) for i, (a, b) in enumerate(zip((*mine, *m_in, *v_in), (*w_s, *m_s, *v_s)))]
    others = [lax.rem(me + d, group) for d in range(1, group)]

    def squares(begin, end, total):
        def body(t, total):
            g = gs[pl.ds(pl.multiple_of(begin + t * unit, unit), unit), :].astype(F32)
            return total + (g * g).reshape(unit // 8, 8, LANES).sum(0)

        return lax.fori_loop(0, (end - begin) // unit, body, total)

    @on_first
    def _():
        for j in others:
            pl.semaphore_signal(pltpu.get_barrier_semaphore(), device_id={axis: j}, device_id_type=MESH)
        for c in sums + loads: c.start()
        dw_s[:] = jnp.zeros_like(dw_s)
        pl.semaphore_wait(pltpu.get_barrier_semaphore(), group - 1)
        for r in big + wo_one: r.start()

    @on_middle
    def _():
        for r in big + wo_one: r.middle()

    project_back(*token_refs, dw_s)

    @on_last
    def _():
        put_columns(dw_s, small, 0, side)
        for r in one: r.start()
        for c in sums: c.wait()
        total = squares(0, early, jnp.zeros(fac.shape, F32))
        for way, r in enumerate(wo_one): r.finish(keeper(way, wide_w, low_w))
        for r in wo_two: r.start()
        for r in one: r.middle()
        for way, r in enumerate(big): r.finish(rounder(way, gs, r.n, early))
        for r in wo_two: r.middle()
        total = squares(early, wo_at, total)
        for way, r in enumerate(one): r.finish(keeper(way, wide_s, low_s))
        for r in two: r.start()
        for way, r in enumerate(wo_two): r.finish(rounder(way, gs, r.n, wo_at))
        total = squares(wo_at, late, total)
        for c in loads: c.wait()
        for r in two: r.middle()
        for way, r in enumerate(two): r.finish(rounder(way, gs, r.n, late))
        sq_all[0] = squares(late, n, total)
        swap = [pltpu.make_async_remote_copy(sq_all.at[0], sq_all.at[d], sq_send.at[d], sq_recv.at[d], device_id={axis: j}, device_id_type=MESH)
                for d, j in enumerate(others, 1)]
        for c in swap: c.start()
        for i, l, c, at, r in blocks_of(segs, 0, n):
            if r == LANES:
                gs[at:at + r, :] = gs[at:at + r, :].astype(F32).T.astype(BF)
        for c in swap: c.wait_recv()
        mean = jnp.sum(sq_all[:].sum(0), keepdims=True) / float(n * LANES * group)
        fac[:] = jnp.broadcast_to(jnp.minimum(1.0, 0.5 * lax.rsqrt(mean + 1e-30)), fac.shape)

        starts = sorted(at for _, _, _, at, _ in blocks_of(segs, 0, n)) + [n]
        cuts = [min(starts, key=lambda r: abs(r - n * t // (2 * parts))) for t in range(2 * parts + 1)]
        spans = list(zip(cuts, cuts[1:]))
        gathers = []
        for c in range(parts):
            for h in BOTH:
                span = spans[h * parts + c]
                for i, l, cs, at, r in blocks_of(segs, *span):
                    g = gs[at:at + r, :].astype(F32) * fac[0:1, :]
                    m, v = m_s[i][l, :, cs], v_s[i][l, :, cs] = moments(m_s[i][l, :, cs], v_s[i][l, :, cs], g)
                    w = w_s[i][l, :, cs].astype(F32)
                    new[at:at + r, :] = (w - lr * (m * lax.rsqrt(v + 1e-8) + 0.1 * w)).astype(BF)
                gathers.append(Gather(sq, h, c * 2 + h, span, new, buf, ag_send, ag_recv))
                gathers[-1].first()
        near, far = (1, 2), 3
        own = pltpu.make_async_copy(new, buf.at[me], own_sem)
        own.start()
        for x in gathers:
            x.pass_first()
            for b in near: x.second(b)
        for x in gathers: x.second(far)
        for x in gathers: x.pass_second(*near)
        for x in gathers: x.second(0)
        for x in gathers: x.pass_second(far)
        for x in gathers: x.pass_second(0)
        for x in gathers: x.end()
        own.wait()
        for c in swap: c.wait_send()


def tail(tokens, wide, low, sums, wo_part, weights, m, v, segs, n, axis, side, parts=3, bm=256):
    dq, _, _, h, *_ = tokens
    t, d = h.shape
    nh, _, hd = dq.shape
    k = len(m)
    group = side * side
    share = [a.shape for a in m]
    unit = share[0][1]
    n_big, n_small = wide.shape[2] * len(BOTH), (nh + 2) * unit
    n_wo = wo_part.shape[2]
    half, half_w = ((len(BOTH), side, x // len(BOTH), LANES) for x in (n_small, n_wo))
    out = [vm((group, n, LANES), BF)] + [vm(s, F32) for s in share] * 2
    room = [sd(a.shape, a.dtype) for a in out]
    return pl.pallas_call(
        functools.partial(_tail, axis=axis, side=side, segs=segs, parts=parts, lr=0.02), name="tail", grid=(t // bm,),
        out_shape=out, in_specs=pre_back_specs(nh, hd, d, bm) + [any_] * (len(sums) + 1 + 3 * k), out_specs=[any_] + [in_vmem] * (2 * k),
        scratch_shapes=[vm(s, BF) for s in share] +
                       [vm((d, (nh + 2) * hd), F32), vm((side, side, n_small, LANES), BF), vm((n, LANES), BF), vm((n, LANES), BF), sem_of(()), vm((group, 8, LANES), F32), vm((8, LANES), F32),
                        vm(half_w, F32), vm(half_w, BF), vm(half, F32), vm(half, BF), sem_of((3 * k,)), sem_of((2,)), sem_of((group,)), sem_of((group,)), *[sem_of((2 * parts, 5, 2, 2))] * 2] +
                       sum((ring_scratch(1, x, unit, F32) for x in (n_big, n_wo, n_small)), []) + sum((ring_scratch(side, x, unit, BF) for x in (n_wo, n_small)), []),
        compiler_params=params(room, **remote(4)),
    )(*tokens, wide, low, *sums, wo_part, *weights, *m, *v)


def _finish(buf_ref, *refs, segs, each):
    (m_in, v_in, w_out), refs = sevens(refs)
    k = len(m_in)
    outs, sem = refs[:-1], refs[-1]
    i = pl.program_id(0)
    stores = [pltpu.make_async_copy(a, b, sem.at[n]) for n, (a, b) in enumerate(zip((*m_in, *v_in), outs))]

    @on_first
    def _():
        for c in stores: c.start()

    for n in range(each):
        for a, l, c, at, r in blocks_of(segs, 0, buf_ref.shape[1]):
            w_out[a][l, n * r:n * r + r, c] = buf_ref[i * each + n, at:at + r, :]

    @on_last
    def _():
        for c in stores: c.wait()


def finish(buf, moments, weights, segs, each=2):
    k = len(moments)
    share = [a.shape for a in moments[:k // 2]]
    return pl.pallas_call(
        functools.partial(_finish, segs=segs, each=each), name="finish", grid=(buf.shape[0] // each,),
        in_specs=[in_vmem] * (1 + k), out_specs=[heads_block(a, b * each, c) for a, b, c in share] + [any_] * k,
        out_shape=[sd(w.shape, BF) for w in weights] + [sd(a.shape, F32) for a in moments],
        scratch_shapes=[sem_of((k,))],
        compiler_params=params([buf, *moments]),
    )(*map(stay, (buf, *moments)))


def solution(mesh):
    axis = "dp"
    group = mesh.shape[axis]
    side = round(group**0.5)

    def step(x, dy, *arrays):
        weights, m, v = (arrays[i : i + 7] for i in (0, 7, 14))
        wq, wk, wv, wo, *mlp = weights
        h0, dy = x[0], dy[0]
        qkv = wq, wk, wv
        head = wk.shape[2]
        scale = head**-0.5
        unit = m[0].shape[1]
        cos, sin = tables(h0.shape[0], head, THETA)
        q0, k0, v0 = pre(h0, cos, sin, *qkv, 0)
        o0, lse0 = attend(q0, k0, v0, scale)
        h1, gate_up, h2, q1, k1, v1 = middle(o0, h0, cos, sin, wo, *mlp, *qkv, 0)
        o1, lse1 = attend(q1, k1, v1, scale)
        dh, do, delta, big, small = mlp_back(o1, h2, dy, wo, *mlp, 1, side, axis, bm=512)
        d1 = attend_back(q1, k1, v1, do, lse1, delta, scale, big, side, axis, unit)
        dh, g1, small = pre_back(*d1, h2, cos, sin, 1, side, axis, small, dh, *qkv)
        _, do, delta, big, wo0, gw1 = mlp_back(o0, h1, dh, wo, *mlp, 0, side, axis, gate_up, small)
        *d0, wide, low = attend_back(q0, k0, v0, do, lse0, delta, scale, big, side, axis, unit)
        wq_, wk_, wv_, wo_, gate_, up_, down_ = range(7)
        order = [(i, l) for l in (1, 0) for i in (gate_, up_, down_, wo_, wq_, wk_, wv_)]
        segs, n = segments([w.shape for w in weights], order, group)
        buf, *moments = tail((*d0, h0, cos, sin), wide, low, (g1, gw1), wo0, weights, m, v, segs, n, axis, side)
        return tuple(finish(buf, moments, weights, segs))

    states, all_of, cut = P(("rep", "dp"), None, None), P(None, None, None), P(None, "dp", None)
    return jax.shard_map(
        step,
        mesh=mesh,
        in_specs=(states, states) + (all_of,) * 7 + (cut,) * 14,
        out_specs=(P("rep", None, None),) * 7 + (P("rep", "dp", None),) * 14,
        check_vma=False,
    )
```

```python
import functools

import jax
import jax.numpy as jnp
from jax import lax
from jax.experimental import pallas as pl
from jax.experimental.pallas import tpu as pltpu
from jax.sharding import PartitionSpec as P

BF, F32 = jnp.bfloat16, jnp.float32
THETA = 10000
LOG2E = 1.4426950408889634
HIDDEN = -1e30
BOTH = range(2)
SIDES = 1, -1


FULL = 63 * 2**20
LANES = 128


MESH = pl.DeviceIdType.MESH
sd, vm, sem_of = jax.ShapeDtypeStruct, pltpu.VMEM, pltpu.SemaphoreType.DMA
any_ = pl.BlockSpec(memory_space=pl.ANY)
in_vmem = pl.BlockSpec(memory_space=pltpu.VMEM)


def remote(n):
    return dict(collective_id=n, has_side_effects=True)


def params(held=(), spare=0, **more):
    room = FULL - spare - sum(a.size * a.dtype.itemsize for a in held)
    return pltpu.CompilerParams(dimension_semantics=("arbitrary",), vmem_limit_bytes=room, **more)


def stay(a):
    return pltpu.with_memory_space_constraint(a, vm)


def heads_block(heads, bm, d):
    return pl.BlockSpec((heads, bm, d), lambda i: (0, i, 0))


def stat_block(heads, bm):
    return pl.BlockSpec((heads, 1, bm), lambda i: (0, 0, i))


def on_first(run):
    pl.when(pl.program_id(0) == 0)(run)


def on_middle(run):
    pl.when(pl.program_id(0) == pl.num_programs(0) // 2)(run)


def on_last(run):
    pl.when(pl.program_id(0) == pl.num_programs(0) - 1)(run)


def iota(shape, axis):
    return lax.broadcasted_iota(jnp.int32, shape, axis)


def lanes(n, size=LANES):
    return slice(n * size, n * size + size)


def dot(a, b, ca=1, cb=0):
    return lax.dot_general(a, b, (((ca,), (cb,)), ((), ())), preferred_element_type=F32)

def mm(a, b):
    return dot(a, b).astype(BF)


def dot_nt(a, b):
    return dot(a, b, 1, 1)


def dot_tn(a, b):
    return dot(a, b, 0, 0)

def sigmoid(g):
    return 1.0 / (1.0 + jnp.exp(-g))


def mean(x):
    return jnp.mean(x, -1, keepdims=True)


def top_of(x):
    return x.max(0, keepdims=True)


def norm_of(h):
    wide = h.astype(F32)
    scale = lax.rsqrt(mean(wide * wide) + 1e-6)
    return wide, scale, (wide * scale).astype(BF)

def norm_back(db, wide, scale):
    return scale * db - wide * (scale * scale * scale * mean(db * wide))

def turn(t, cos, sin):
    return t * cos + pltpu.roll(t, t.shape[1] // 2, 1) * sin

def tables(tokens, head, theta):
    half = head // 2
    rate = theta ** (-jnp.arange(half, dtype=F32) / half)
    low = 64
    a = (jnp.arange(tokens // low, dtype=F32) * low)[:, None] * rate
    b = jnp.arange(low, dtype=F32)[:, None] * rate
    ca, sa, cb, sb = (f(t) for t in (a, b) for f in (jnp.cos, jnp.sin))
    ca, sa, cb, sb = ca[:, None], sa[:, None], cb[None], sb[None]
    cos, sin = (ca * cb - sa * sb).reshape(tokens, half), (sa * cb + ca * sb).reshape(tokens, half)
    return jnp.concatenate([cos, cos], 1), jnp.concatenate([-sin, sin], 1)

def whole(a, layer=None):
    one = layer is not None
    return pl.BlockSpec((None,) * one + a.shape[one:], lambda *_: (layer,) * one + (0,) * (a.ndim - one), pipeline_mode=pl.Buffered(1))

def rows(bm, width):
    return pl.BlockSpec((bm, width), lambda i: (i, 0))

def heads_of(ref):
    return jnp.concatenate([ref[n] for n in range(ref.shape[0])], axis=1)

def project(a, wq, wk, wv, cos, sin, q_ref, k_ref, v_ref):
    hd = cos.shape[1]
    q = mm(a, wq).astype(F32)
    for n in range(q.shape[1] // hd):
        q_ref[n] = turn(q[:, lanes(n, hd)], cos, sin).astype(BF)
    k_ref[:] = turn(mm(a, wk).astype(F32), cos, sin).astype(BF)
    v_ref[:] = mm(a, wv)

def _pre(h_ref, cos_ref, sin_ref, wq, wk, wv, q_ref, k_ref, v_ref):
    _, _, a = norm_of(h_ref[:])
    project(a, wq[:], wk[:], wv[:], cos_ref[:], sin_ref[:], q_ref, k_ref, v_ref)

def pre(h, cos, sin, wq, wk, wv, layer, bm=512):
    t, d = h.shape
    hd = cos.shape[1]
    nh = wq.shape[2] // hd
    return pl.pallas_call(
        _pre, name="pre", grid=(t // bm,),
        in_specs=[rows(bm, d), rows(bm, hd), rows(bm, hd), whole(wq, layer), whole(wk, layer), whole(wv, layer)],
        out_specs=[heads_block(nh, bm, hd), rows(bm, hd), rows(bm, hd)],
        out_shape=[sd((nh, t, hd), BF), sd((t, hd), BF), sd((t, hd), BF)],
        compiler_params=params(),
    )(h, cos, sin, wq, wk, wv)

def fetch(pairs, sem):
    return [pltpu.make_async_copy(a, b, sem.at[n]) for n, (a, b) in enumerate(pairs)]

def _mid(o_ref, h_ref, cos_ref, sin_ref, wo, wg, wu, wd, wq, wk, wv, h1_ref, gu_ref, h2_ref, q_ref, k_ref, v_ref,
         wo_s, wg_s, wu_s, wd_s, wq_s, wk_s, wv_s, sem, *, layer, part):
    i = pl.program_id(0)
    cps = fetch([(a.at[layer], b) for a, b in ((wo, wo_s), (wg, wg_s), (wu, wu_s), (wd, wd_s))] +
                [(a.at[layer + 1], b) for a, b in ((wq, wq_s), (wk, wk_s), (wv, wv_s))], sem)

    @on_first
    def _():
        for c in cps: c.start()
        cps[0].wait()

    h1 = h_ref[:] + mm(heads_of(o_ref), wo_s[:])
    h1_ref[:] = h1
    _, _, b = norm_of(h1)

    @on_first
    def _():
        for c in cps[1:]: c.wait()

    f = wg_s.shape[1]
    y = None
    for at in range(0, f, part):
        c = slice(at, at + part)
        g, u = dot(b, wg_s[:, c]), dot(b, wu_s[:, c])
        gu_ref[:, c] = g
        gu_ref[:, f + at:f + at + part] = u
        act = (g * sigmoid(g) * u).astype(BF)
        yc = dot(act, wd_s[c, :])
        y = yc if y is None else y + yc
    h2 = h1 + y.astype(BF)
    h2_ref[:] = h2
    _, _, a = norm_of(h2)
    project(a, wq_s[:], wk_s[:], wv_s[:], cos_ref[:], sin_ref[:], q_ref, k_ref, v_ref)

def middle(o, h, cos, sin, wo, wg, wu, wd, wq, wk, wv, layer, bm=512, part=512):
    t, d = h.shape
    nh, _, hd = o.shape
    f = wg.shape[2]
    hs = heads_block(nh, bm, hd)
    return pl.pallas_call(
        functools.partial(_mid, layer=layer, part=part), name="middle", grid=(t // bm,),
        in_specs=[hs, rows(bm, d), rows(bm, hd), rows(bm, hd)] + [any_] * 7,
        out_specs=[rows(bm, d), rows(bm, 2 * f), rows(bm, d), hs, rows(bm, hd), rows(bm, hd)],
        out_shape=[sd((t, d), BF), sd((t, 2 * f), F32), sd((t, d), BF), sd((nh, t, hd), BF), sd((t, hd), BF), sd((t, hd), BF)],
        scratch_shapes=[vm(w.shape[1:], BF) for w in (wo, wg, wu, wd, wq, wk, wv)] + [sem_of((7,))],
        compiler_params=params(),
    )(o, h, cos, sin, wo, wg, wu, wd, wq, wk, wv)


class Square:
    def __init__(self, axis, side):
        self.axis, self.side = axis, side
        me = lax.axis_index(axis)
        self.me = me
        self.place = lax.div(me, side), lax.rem(me, side)

    def at(self, way, along, across=0):
        x, y = (lax.rem(p + (along if n == way else across) + self.side, self.side) for n, p in enumerate(self.place))
        return x * self.side + y

    def greet(self):
        for way in BOTH:
            for step in SIDES:
                pl.semaphore_signal(pltpu.get_barrier_semaphore(), device_id={self.axis: self.at(way, step)}, device_id_type=MESH)

    def met(self):
        pl.semaphore_wait(pltpu.get_barrier_semaphore(), 4)


class Ring:
    KINDS = "far", "free", "joined"

    def __init__(self, sq, way, send, keep, n, unit, s):
        self.sq, self.way, self.send, self.keep, self.unit = sq, way, send, keep, unit
        self.first, self.final, self.mid, self.own, self.out, self.send_sem, self.recv_sem, self.sem, self.own_sem = s
        cut = n // unit // 2 * unit
        self.halves = (0, cut), (cut, n - cut)
        self.n = n

    @staticmethod
    def scratch(k, n, unit, kept):
        most = n - n // unit // 2 * unit
        part, full = (len(BOTH), k, most, LANES), (k, n, LANES)
        return [vm(part, BF), vm((len(BOTH), *full), BF), vm(part, kept), vm(full, kept), vm(part, BF)] + [sem_of((3, len(BOTH)))] * 2 + [sem_of((len(BOTH),)), sem_of(())]

    def block(self, step):
        return lax.rem(self.sq.place[self.way] + step + self.sq.side, self.sq.side)

    def copy(self, kind, d):
        half = 1 - d if kind == "free" else d
        rows, size = pl.ds(*self.halves[half]), pl.ds(0, self.halves[half][1])
        src = self.out.at[d, :, size] if kind == "joined" else self.send(self.block(2 if kind == "far" else SIDES[d]), rows)
        dst = self.first.at[d, :, size] if kind == "far" else self.final.at[d, :, rows]
        n = self.KINDS.index(kind), d
        to = {self.sq.axis: self.sq.at(self.way, SIDES[d])}
        return pltpu.make_async_remote_copy(src, dst, self.send_sem.at[n], self.recv_sem.at[n], device_id=to, device_id_type=MESH)

    def added(self, d):
        rows, size = pl.ds(*self.halves[d]), self.halves[d][1]
        return pltpu.make_async_copy(self.keep(self.block(SIDES[d]), rows), self.mid.at[d, :, pl.ds(0, size)], self.sem.at[d])

    def mine(self):
        return pltpu.make_async_copy(self.keep(self.block(0), pl.ds(0, self.n)), self.own, self.own_sem)

    def start(self):
        for kind in self.KINDS[:2]:
            for d in BOTH:
                self.copy(kind, d).start()
        for d in BOTH:
            self.added(d).start()
        self.mine().start()

    def steps(self, size, run):
        def body(t, _):
            run(pl.ds(pl.multiple_of(t * self.unit, self.unit), self.unit))
            return _

        lax.fori_loop(0, size // self.unit, body, 0)

    def middle(self):
        for d in BOTH:
            self.copy("far", d).wait_recv()
            self.added(d).wait()

            def add(here, d=d):
                self.out[d, :, here] = (self.mid[d, :, here].astype(F32) + self.first[d, :, here].astype(F32)).astype(BF)

            self.steps(self.halves[d][1], add)
            self.copy("joined", d).start()

    def finish(self, put):
        for d in BOTH:
            for kind in self.KINDS[1:]:
                self.copy(kind, d).wait_recv()
        self.mine().wait()
        self.steps(self.n, lambda here: put(here, self.own[:, here].astype(F32) + sum(self.final[d, :, here].astype(F32) for d in BOTH)))
        for d in BOTH:
            for kind in self.KINDS:
                self.copy(kind, d).wait_send()


def first_rings(sq, g, unit, scr):
    n = g.shape[2] // 2
    x_block = lambda p, rows: g.at[p, :, rows]
    y_block = lambda p, rows: g.at[:, p, pl.ds(rows.start + n, rows.size)]
    return [Ring(sq, way, block, block, n, unit, scr[way]) for way, block in enumerate((x_block, y_block))]


def second_rings(sq, wide, low, unit, scr):
    pick = lambda ref, way: (lambda p, rows: ref.at[way, pl.ds(p, 1), rows])
    return [Ring(sq, 1 - way, pick(low, way), pick(wide, way), wide.shape[2], unit, scr[way]) for way in BOTH]


def ring_scratch(k, n, unit, kept):
    return Ring.scratch(k, n // 2, unit, kept) * 2


def pairs(scr):
    half = len(scr) // 2
    return scr[:half], scr[half:]


def keeper(way, wide, low):
    def put(rows, total):
        wide[way, :, rows] = total
        low[way, :, rows] = total.astype(BF)
    return put


def rounder(way, g, n, at=0):
    def put(rows, total):
        g[pl.ds(pl.multiple_of(rows.start + (at + way * n), 16), rows.size)] = total[0].astype(BF)
    return put


def leave(sq, way, ring, low, wide, sem):
    q, side = sq.place[1 - way], sq.side
    full, (one, other) = pl.ds(0, ring.n), (pl.ds(*h) for h in ring.halves)
    got = []
    for pair, parts in ((wide, (full, one, None, other)), (low, (None, other, full, one))):
        for step, part in enumerate(parts):
            if part:
                at = way, lax.rem(q + step, side), part
                got.append(pltpu.make_async_copy(pair[0].at[at], pair[1].at[at], sem.at[len(got)]))
                got[-1].start()
    return got


def _attend(q_ref, k_ref, v_ref, o_ref, lse_ref, s_a, s_b, top_a, top_b, vt_s, gap_s, *, scale, bq):
    heads, _, d = q_ref.shape
    tokens = k_ref.shape[0]
    iq = pl.program_id(0)
    e = scale * LOG2E

    @on_first
    def _():
        vt_s[:d, :] = v_ref[:].astype(F32).T.astype(BF)
        vt_s[d:, :] = jnp.ones_like(vt_s[d:, :])
        gap_s[:] = iota(gap_s.shape, 1) - iota(gap_s.shape, 0)

    half = bq // 2

    def score(n, keys, s_ref, top_ref):
        q = q_ref[n]
        cut = keys - half
        top = None
        if keys > bq:
            s = dot_nt(k_ref[:keys - bq, :], q)
            s_ref[:keys - bq, :] = s
            top = top_of(s)
        near = dot_nt(k_ref[keys - bq:cut, :], q)
        left = jnp.where(gap_s[:] >= 0, near[:, :half], HIDDEN)
        right = near[:, half:]
        s_ref[keys - bq:cut, :half] = left
        s_ref[keys - bq:cut, half:] = right
        far = jnp.where(gap_s[:] >= 0, dot_nt(k_ref[cut:keys, :], q[half:, :]), HIDDEN)
        s_ref[cut:keys, half:] = far
        m = jnp.concatenate([top_of(left), jnp.maximum(top_of(right), top_of(far))], 1)
        top_ref[:] = m if top is None else jnp.maximum(m, top)

    def weigh(n, keys, s_ref, top_ref):
        cut = keys - half
        top = top_ref[:]
        pa = jnp.exp2((s_ref[:cut, :] - top) * e).astype(BF)
        pb = jnp.exp2((s_ref[cut:keys, half:] - top[:, half:]) * e).astype(BF)
        mix = dot(vt_s[:, :cut], pa)
        more = dot(vt_s[:, cut:keys], pb)
        mix = jnp.concatenate([mix[:, :half], mix[:, half:] + more], 1)
        total = mix[d:d + 1, :]
        o_ref[n] = (mix[:d, :] * (1.0 / total)).T.astype(o_ref.dtype)
        lse_ref[n] = top * scale + jnp.log(total)

    for j in range(tokens // bq):
        @pl.when(iq == j)
        def _(keys=(j + 1) * bq):
            score(0, keys, s_a, top_a)

            def pair(t, _):
                score(2 * t + 1, keys, s_b, top_b)
                weigh(2 * t, keys, s_a, top_a)
                score(2 * t + 2, keys, s_a, top_a)
                weigh(2 * t + 1, keys, s_b, top_b)
                return _

            lax.fori_loop(0, heads // 2 - 1, pair, 0)
            score(heads - 1, keys, s_b, top_b)
            weigh(heads - 2, keys, s_a, top_a)
            weigh(heads - 1, keys, s_b, top_b)

def attend(q, k, v, scale, bq=512):
    heads, tokens, d = q.shape
    here = heads_block(heads, bq, d)
    all_ = whole(k)
    return pl.pallas_call(
        functools.partial(_attend, scale=scale, bq=bq), name="attend", grid=(tokens // bq,),
        in_specs=[here, all_, all_],
        out_specs=[here, stat_block(heads, bq)],
        out_shape=[sd(q.shape, BF), sd((heads, 1, tokens), F32)],
        scratch_shapes=[vm((tokens, bq), F32), vm((tokens, bq), F32), vm((1, bq), F32), vm((1, bq), F32),
                        vm((d + 8, tokens), BF), vm((bq // 2, bq // 2), jnp.int32)],
        compiler_params=params(),
    )(q, k, v)
def _attend_back(q_ref, k_ref, v_ref, do_ref, lse_ref, delta_ref, g_ref, dq_ref, dk_ref, dv_ref, wide_ref, low_ref,
                 s_a, s_b, dp_a, dp_b, kt_s, vt_s, dkt_s, dvt_s, gap_s, wide_s, low_s, sem, *scr, scale, bq, side, axis, unit):
    heads, _, d = q_ref.shape
    tokens = k_ref.shape[0]
    iq = pl.program_id(0)
    e = scale * LOG2E
    half = bq // 2

    sq = Square(axis, side)
    rings = first_rings(sq, g_ref, unit, pairs(scr))
    last = pl.num_programs(0) - 1

    @on_first
    def _():
        sq.greet()
        row = iota((d, tokens), 0)
        kt_s[:d, :] = k_ref[:].astype(F32).T.astype(BF)
        kt_s[d:, :] = jnp.where(row < 3, 1.0, 0.0).astype(BF)
        vt_s[:d, :] = v_ref[:].astype(F32).T.astype(BF)
        vt_s[d:, :] = jnp.where((row >= 3) & (row < 6), 1.0, 0.0).astype(BF)
        gap_s[:] = iota(gap_s.shape, 0) - iota(gap_s.shape, 1)
        dkt_s[:] = jnp.zeros_like(dkt_s)
        dvt_s[:] = jnp.zeros_like(dvt_s)
        sq.met()
        for r in rings: r.start()

    @on_last
    def _():
        for r in rings: r.middle()

    def parts(x):
        a = x.astype(BF).astype(F32)
        b = (x - a).astype(BF).astype(F32)
        return [a, b, x - a - b]

    def score(n, keys, s_ref, dp_ref):
        cut = keys - half
        row = iota((d, bq), 0)
        rows = jnp.zeros((d, bq), F32)
        for i, x in enumerate(parts(lse_ref[n] * (-1 / scale)) + parts(-delta_ref[n])):
            rows = jnp.where(row == i, x, rows)
        extra = rows.T.astype(BF)
        q = jnp.concatenate([q_ref[n], extra], 1)
        do = jnp.concatenate([do_ref[n], extra], 1)
        if keys > bq:
            s_ref[:, :keys - bq] = dot(q, kt_s[:, :keys - bq])
        near = dot(q, kt_s[:, keys - bq:cut])
        s_ref[:half, keys - bq:cut] = jnp.where(gap_s[:] >= 0, near[:half], HIDDEN)
        s_ref[half:, keys - bq:cut] = near[half:]
        s_ref[half:, cut:keys] = jnp.where(gap_s[:] >= 0, dot(q[half:], kt_s[:, cut:keys]), HIDDEN)
        dp_ref[:, :cut] = dot(do, vt_s[:, :cut])
        dp_ref[half:, cut:keys] = dot(do[half:], vt_s[:, cut:keys])

    def weigh(n, keys, s_ref, dp_ref):
        cut = keys - half
        qt = q_ref[n].astype(F32).T.astype(BF)
        dot_ = do_ref[n].astype(F32).T.astype(BF)
        pa = jnp.exp2(s_ref[:, :cut] * e)
        da = (pa * dp_ref[:, :cut]).astype(BF)
        pb = jnp.exp2(s_ref[half:, cut:keys] * e)
        db = (pb * dp_ref[half:, cut:keys]).astype(BF)
        dvt_s[:, :cut] += dot(dot_, pa.astype(BF))
        dkt_s[:, :cut] += dot(qt, da)
        dvt_s[:, cut:keys] += dot(dot_[:, half:], pb.astype(BF))
        dkt_s[:, cut:keys] += dot(qt[:, half:], db)
        dq = dot(da, k_ref[:cut, :])
        far = dot(db, k_ref[cut:keys, :])
        dq_ref[n, :half] = (dq[:half] * scale).astype(BF)
        dq_ref[n, half:] = ((dq[half:] + far) * scale).astype(BF)

    for j in range(tokens // bq):
        @pl.when(iq == j)
        def _(keys=(j + 1) * bq):
            score(0, keys, s_a, dp_a)

            def pair(t, _):
                score(2 * t + 1, keys, s_b, dp_b)
                weigh(2 * t, keys, s_a, dp_a)
                score(jnp.minimum(2 * t + 2, heads - 1), keys, s_a, dp_a)
                weigh(2 * t + 1, keys, s_b, dp_b)
                return _

            lax.fori_loop(0, heads // 2, pair, 0)

    @on_last
    def _():
        outs = []
        for way, r in enumerate(rings):
            r.finish(keeper(way, wide_s, low_s))
            outs += leave(sq, way, r, (low_s, low_ref), (wide_s, wide_ref), sem.at[way])
        dk_ref[:] = (dkt_s[:] * scale).T.astype(BF)
        dv_ref[:] = dvt_s[:].T.astype(BF)
        for c in outs: c.wait()

def attend_back(q, k, v, do, lse, delta, scale, g, side, axis, unit, bq=512):
    n = g.shape[2]
    half = (2, side, n // 2, LANES)
    heads, tokens, d = q.shape
    here = heads_block(heads, bq, d)
    all_ = whole(k)
    stat = stat_block(heads, bq)
    return pl.pallas_call(
        functools.partial(_attend_back, scale=scale, bq=bq, side=side, axis=axis, unit=unit), name="attend_back", grid=(tokens // bq,),
        in_specs=[here, all_, all_, here, stat, stat, any_],
        out_specs=[here, all_, all_, any_, any_],
        out_shape=[sd(q.shape, BF)] + [sd(k.shape, BF)] * 2 + [sd(half, F32), sd(half, BF)],
        scratch_shapes=[vm((bq, tokens), F32)] * 4 + [vm((2 * d, tokens), BF)] * 2 + [vm((d, tokens), F32)] * 2 +
                       [vm((bq // 2, bq // 2), jnp.int32), vm(half, F32), vm(half, BF), sem_of((2, 6))] + ring_scratch(side, n, unit, BF),
        compiler_params=params(**remote(1)),
    )(q, k, v, do, lse, delta, g)


def split_rows(x, side, r):
    return x.astype(BF).reshape(side, side, r, x.shape[1])


def put_columns(acc, stage, at, side):
    r = acc.shape[0] // (side * side)
    for cb in range(acc.shape[1] // LANES):
        stage[:, :, at:at + r, :] = split_rows(acc[:, lanes(cb)], side, r)
        at += r
    return at


def sync(a, b, sem):
    c = pltpu.make_async_copy(a, b, sem.at[0])
    c.start()
    c.wait()


def copy_rows(stage, out, at, sem):
    c = pltpu.make_async_copy(stage, out.at[:, :, pl.ds(at, stage.shape[2])], sem)
    c.start()
    return c


def mlp_body(i, o, h1, dy, gu, w, acc, dh_ref, do_ref, delta_ref, part):
    wo_s, wg_s, wu_s, wd_s = w
    dwg_s, dwu_s, dwd_s, dwo_s = acc
    heads, _, hd = do_ref.shape
    wide, scale, b = norm_of(h1)
    db = None
    for at in range(0, wg_s.shape[1], part):
        c = slice(at, at + part)
        g, u = gu(c) if gu else (dot(b, wg_s[:, c]), dot(b, wu_s[:, c]))
        da = dot_nt(dy, wd_s[c, :]).astype(BF).astype(F32)
        s = sigmoid(g)
        silu = g * s
        act = (silu * u).astype(BF)
        du = (da * silu).astype(BF)
        dg = (da * u * (s + silu * (1.0 - s))).astype(BF)
        dbc = dot_nt(dg, wg_s[:, c]) + dot_nt(du, wu_s[:, c])
        db = dbc if db is None else db + dbc
        dwg_s[:, c] += dot_tn(b, dg)
        dwu_s[:, c] += dot_tn(b, du)
        dwd_s[:, c] += dot_tn(dy, act)
    dh = dy + norm_back(db.astype(BF).astype(F32), wide, scale).astype(BF)
    dh_ref[:] = dh
    do = dot_nt(dh, wo_s[:]).astype(BF)
    prod = do.astype(F32) * o.astype(F32)
    lane = iota((dy.shape[0], LANES), 1)
    table = jnp.zeros((dy.shape[0], LANES), F32)
    for n in range(heads):
        c = lanes(n, hd)
        do_ref[n] = do[:, c]
        table = jnp.where(lane == n, jnp.sum(prod[:, c], -1, keepdims=True), table)
    table = table.T
    for n in range(heads):
        delta_ref[n] = table[n:n + 1, :]
    dwo_s[:] += dot_tn(o, dh)


def _mlp_back(*refs, layer, part, side, axis, kept):
    i, steps = pl.program_id(0), pl.num_programs(0)
    o_ref, h_ref, dy_ref, *refs = refs
    if kept:
        gu_ref, *refs = refs
    wo, wg, wu, wd, *refs = refs
    if kept:
        early, *refs = refs
    dh_ref, do_ref, delta_ref, big, small, *refs = refs
    if kept:
        g_out, *refs = refs
    wo_s, wg_s, wu_s, wd_s, dwg_s, dwu_s, dwd_s, dwo_s, st_a, st_b, sem, sem_a, sem_b, *refs = refs
    w, acc = (wo_s, wg_s, wu_s, wd_s), (dwg_s, dwu_s, dwd_s, dwo_s)
    cps = [pltpu.make_async_copy(a.at[layer], b, sem.at[n]) for n, (a, b) in enumerate(zip((wo, wg, wu, wd), w))]
    if kept:
        wide_s, low_s, g_s, *scr = refs
        sq = Square(axis, side)
        unit = dh_ref.shape[1] // (side * side)
        half = len(scr) // 2
        one = first_rings(sq, early, unit, pairs(scr[:half]))
        two = second_rings(sq, wide_s, low_s, unit, pairs(scr[half:]))

    @on_first
    def _():
        for c in cps: c.start()
        if kept: sq.greet()
        for r in acc: r[:] = jnp.zeros_like(r)
        if kept:
            sq.met()
            for r in one: r.start()
        for c in cps: c.wait()

    if kept:
        @pl.when(i == steps // 2 - 1)
        def _():
            for r in one: r.middle()

        @pl.when(i == steps // 2 + 1)
        def _():
            for way, r in enumerate(one): r.finish(keeper(way, wide_s, low_s))
            for r in two: r.start()

        @on_last
        def _():
            for r in two: r.middle()

    o, dy = heads_of(o_ref), dy_ref[:]
    if kept:
        f = gu_ref.shape[1] // 2
        mlp_body(i, o, h_ref[:], dy, lambda c: (gu_ref[:, c], gu_ref[:, c.start + f:c.stop + f]), w, acc, dh_ref, do_ref, delta_ref, part)
    else:
        mlp_body(i, o, h_ref[:] + mm(o, wo_s[:]), dy, None, w, acc, dh_ref, do_ref, delta_ref, part)

    @on_last
    def _():
        n = st_a.shape[2]
        put_columns(dwg_s, st_a, 0, side)
        first = copy_rows(st_a, big, 0, sem_a)
        put_columns(dwu_s, st_b, 0, side)
        second = copy_rows(st_b, big, n, sem_b)
        first.wait()
        for x in range(side):
            for y in range(side):
                st_a[x, y] = dwd_s[:, lanes(x * side + y)].astype(BF)
        third = copy_rows(st_a, big, 2 * n, sem_a)
        second.wait()
        size = put_columns(dwo_s, st_b, 0, side)
        fourth = copy_rows(st_b.at[:, :, pl.ds(0, size)], small, 0, sem_b)
        if kept:
            for way, r in enumerate(two): r.finish(rounder(way, g_s, r.n))
            sync(g_s, g_out, sem)
        third.wait()
        fourth.wait()


def mlp_back(o, h, dy, wo, wg, wu, wd, layer, side, axis, gu=None, early=None, bm=256, part=1024):
    t, d = h.shape
    nh, _, hd = o.shape
    f = wg.shape[2]
    kept = gu is not None
    hs = heads_block(nh, bm, hd)
    unit = d // (side * side)
    n_wo = d // LANES * unit
    n_own = n_wo if kept else n_wo + (nh + 2) * unit
    n_small = early.shape[2] if kept else 0
    given = [o, h, dy] + [gu] * kept + [wo, wg, wu, wd] + [early] * kept
    half = n_small // 2
    return pl.pallas_call(
        functools.partial(_mlp_back, layer=layer, part=part, side=side, axis=axis, kept=kept), name=f"mlp_back{layer}", grid=(t // bm,),
        in_specs=[hs, rows(bm, d), rows(bm, d)] + [rows(bm, 2 * f)] * kept + [any_] * (4 + kept),
        out_specs=[rows(bm, d), hs, stat_block(nh, bm)] + [any_] * (2 + kept),
        out_shape=[sd((t, d), BF), sd((nh, t, hd), BF), sd((nh, 1, t), F32), sd((side, side, 3 * d, LANES), BF), sd((side, side, n_own, LANES), BF)] +
                  [sd((n_small, LANES), BF)] * kept,
        scratch_shapes=[vm(w.shape[1:], BF) for w in (wo, wg, wu, wd)] + [vm((d, f), F32)] * 3 + [vm((d, d), F32)] + [vm((side, side, d, LANES), BF)] * 2 +
                       [sem_of((4,)), sem_of(()), sem_of(())] +
                       ([vm((2, side, half, LANES), F32), vm((2, side, half, LANES), BF), vm((n_small, LANES), BF)] +
                        ring_scratch(side, n_small, unit, BF) + ring_scratch(1, n_small, unit, F32) if kept else []),
        compiler_params=params(**(remote(3) if kept else {})),
    )(*given)


def project_back(dq_ref, dk_ref, dv_ref, h_ref, cos_ref, sin_ref, dw_s):
    cos, sin = cos_ref[:], -sin_ref[:]
    wide, scale, a = norm_of(h_ref[:])
    dk = turn(dk_ref[:].astype(F32), cos, sin).astype(BF)
    dq = jnp.concatenate([turn(dq_ref[n].astype(F32), cos, sin).astype(BF) for n in range(dq_ref.shape[0])], 1)
    ds = dq, dk, dv_ref[:]
    dw_s[:] += dot_tn(a, jnp.concatenate(ds, 1))
    return wide, scale, ds


def _pre_back(dq_ref, dk_ref, dv_ref, h_ref, cos_ref, sin_ref, wide, low, dh_ref, wq, wk, wv, _, out_dh, g_out, out, dw_s, stage,
              out_sem, sem, g_s, *scr, side, axis):
    sq = Square(axis, side)
    rings = second_rings(sq, wide, low, h_ref.shape[1] // (side * side), pairs(scr))

    @on_first
    def _():
        sq.greet()
        dw_s[:] = jnp.zeros_like(dw_s)
        sq.met()
        for r in rings: r.start()

    @on_middle
    def _():
        for r in rings: r.middle()

    wide_h, scale, ds = project_back(dq_ref, dk_ref, dv_ref, h_ref, cos_ref, sin_ref, dw_s)
    da = sum(dot_nt(d, w[:]) for d, w in zip(ds, (wq, wk, wv)))
    out_dh[:] = dh_ref[:] + norm_back(da.astype(BF).astype(F32), wide_h, scale).astype(BF)

    @on_last
    def _():
        put_columns(dw_s, stage, 0, side)
        c = copy_rows(stage, out, out.shape[2] - stage.shape[2], out_sem)
        for way, r in enumerate(rings): r.finish(rounder(way, g_s, r.n))
        sync(g_s, g_out, sem)
        c.wait()


def pre_back_specs(nh, hd, d, bm):
    return [heads_block(nh, bm, hd), rows(bm, hd), rows(bm, hd), rows(bm, d), rows(bm, hd), rows(bm, hd), any_, any_]


def pre_back(dq, dk, dv, wide, low, h, cos, sin, layer, side, axis, small, dh, *ws, bm=512):
    t, d = h.shape
    nh, _, hd = dq.shape
    unit = d // (side * side)
    packed = side, side, (nh + 2) * unit, LANES
    n = wide.shape[2] * len(BOTH)
    return pl.pallas_call(
        functools.partial(_pre_back, side=side, axis=axis), name="pre_back", grid=(t // bm,),
        in_specs=pre_back_specs(nh, hd, d, bm) + [rows(bm, d)] + [whole(w, layer) for w in ws] + [any_],
        out_specs=[rows(bm, d)] + [any_] * 2,
        out_shape=[sd((t, d), BF), sd((n, LANES), BF), sd(small.shape, BF)],
        input_output_aliases={9 + len(ws): 2},
        scratch_shapes=[vm((d, (nh + 2) * hd), F32), vm(packed, BF), sem_of(()), sem_of((1,)), vm((n, LANES), BF)] + ring_scratch(1, n, unit, F32),
        compiler_params=params(**remote(2)),
    )(dq, dk, dv, h, cos, sin, wide, low, dh, *ws, small)


def segments(shapes, order, group):
    out, at = [], 0
    for i, l in order:
        r, c = shapes[i][1] // group, shapes[i][2]
        out.append((i, l, r, c, at))
        at += r * c // LANES
    return out, at


def moments(m, v, g):
    return 0.9 * m + 0.1 * g, 0.95 * v + 0.05 * g * g


def blocks_of(segs, begin, end):
    for i, l, r, c, at in segs:
        for cb in range(c // LANES):
            if begin <= at + cb * r < end:
                yield i, l, lanes(cb), at + cb * r, r


def sevens(refs, k=7):
    return [refs[i * k:i * k + k] for i in range(3)], refs[3 * k:]


class Gather:
    ALONG = 0, -1, 1, 2

    def __init__(self, sq, way, part, span, new, buf, send_sem, recv_sem):
        self.sq, self.way, self.part, self.new, self.buf, self.sems, self.sent = sq, way, part, new, buf, (send_sem, recv_sem), []
        begin, end = span
        mid = begin + (end - begin) // 32 * 16
        self.spans = (begin, end - begin), (begin, mid - begin), (mid, end - mid)

    def copy(self, m, source, to, which):
        along, across = source
        owner = self.sq.at(self.way, along, across)
        rows = pl.ds(*self.spans[which])
        place = self.buf.at[owner, rows]
        s, r = (x.at[self.part, *m] for x in self.sems)
        mine = source == (0, 0)
        return pltpu.make_async_remote_copy(self.new.at[rows] if mine else place, place, s, r, device_id={self.sq.axis: self.sq.at(self.way, *to)}, device_id_type=MESH)

    def go(self, *a, **k):
        c = self.copy(*a, **k)
        c.start()
        self.sent.append(c)

    def got(self, m, source, which):
        self.copy(m, source, (1, 0), which).wait_recv()

    def first(self):
        for m, to in enumerate(SIDES):
            self.go((0, 0, m), (0, 0), (to, 0), 0)

    def pass_first(self):
        for m, to in enumerate(SIDES):
            self.got((0, 0, m), (-to, 0), 0)
            self.go((0, 1, m), (-to, 0), (to, 0), 1 + m)

    def second(self, b):
        along = self.ALONG[b]
        for m, to in enumerate(SIDES):
            if along == 2:
                self.got((0, 1, m), (along, 0), 1 + m)
        for m, to in enumerate(SIDES):
            self.go((1 + b, 0, m), (along, 0), (0, to), 0)

    def pass_second(self, *bs):
        for b in bs:
            along = self.ALONG[b]
            for m, to in enumerate(SIDES):
                self.got((1 + b, 0, m), (along, -to), 0)
                self.go((1 + b, 1, m), (along, -to), (0, to), 1 + m)

    def end(self):
        for b, along in enumerate(self.ALONG):
            for m in BOTH:
                self.got((1 + b, 1, m), (along, 2), 1 + m)
        for c in self.sent: c.wait_send()


def _tail(*refs, axis, side, segs, parts, lr):
    *token_refs, wide, low, g1, gw1, wo_ref = refs[:11]
    (w_in, m_in, v_in), refs = sevens(refs[11:])
    buf, *refs = refs
    (m_s, v_s, w_s), refs = sevens(refs)
    dw_s, small, gs, new, own_sem, sq_all, fac, wide_w, low_w, wide_s, low_s, in_sem, g_sem, sq_send, sq_recv, ag_send, ag_recv, *scr = refs
    part = len(scr) // 5
    ring_s = [pairs(scr[i:i + part]) for i in range(0, len(scr), part)]
    group = side * side
    n = gs.shape[0]
    sq = Square(axis, side)
    me = sq.me
    unit = m_s[0].shape[1]
    early = g1.shape[0] + gw1.shape[0]
    late = n - small.shape[2]
    big, wo_two, two = (second_rings(sq, a, b, unit, r) for a, b, r in zip((wide, wide_w, wide_s), (low, low_w, low_s), ring_s))
    wo_one, one = (first_rings(sq, a, unit, r) for a, r in zip((wo_ref, small), ring_s[3:]))
    wo_at = late - wo_ref.shape[2]
    sums = [pltpu.make_async_copy(a, gs.at[pl.ds(at, a.shape[0])], g_sem.at[i]) for i, (a, at) in enumerate(((g1, 0), (gw1, g1.shape[0])))]
    mine = [w.at[:, pl.ds(pl.multiple_of(me * m.shape[1], m.shape[1]), m.shape[1]), :] for w, m in zip(w_in, m_s)]
    loads = [pltpu.make_async_copy(a, b, in_sem.at[i]) for i, (a, b) in enumerate(zip((*mine, *m_in, *v_in), (*w_s, *m_s, *v_s)))]
    others = [lax.rem(me + d, group) for d in range(1, group)]

    def squares(begin, end, total):
        def body(t, total):
            g = gs[pl.ds(pl.multiple_of(begin + t * unit, unit), unit), :].astype(F32)
            return total + (g * g).reshape(unit // 8, 8, LANES).sum(0)

        return lax.fori_loop(0, (end - begin) // unit, body, total)

    @on_first
    def _():
        for j in others:
            pl.semaphore_signal(pltpu.get_barrier_semaphore(), device_id={axis: j}, device_id_type=MESH)
        for c in sums + loads: c.start()
        dw_s[:] = jnp.zeros_like(dw_s)
        pl.semaphore_wait(pltpu.get_barrier_semaphore(), group - 1)
        for r in big + wo_one: r.start()

    @on_middle
    def _():
        for r in big + wo_one: r.middle()

    project_back(*token_refs, dw_s)

    @on_last
    def _():
        put_columns(dw_s, small, 0, side)
        for r in one: r.start()
        for c in sums: c.wait()
        total = squares(0, early, jnp.zeros(fac.shape, F32))
        for way, r in enumerate(wo_one): r.finish(keeper(way, wide_w, low_w))
        for r in wo_two: r.start()
        for r in one: r.middle()
        for way, r in enumerate(big): r.finish(rounder(way, gs, r.n, early))
        for r in wo_two: r.middle()
        total = squares(early, wo_at, total)
        for way, r in enumerate(one): r.finish(keeper(way, wide_s, low_s))
        for r in two: r.start()
        for way, r in enumerate(wo_two): r.finish(rounder(way, gs, r.n, wo_at))
        total = squares(wo_at, late, total)
        for c in loads: c.wait()
        for r in two: r.middle()
        for way, r in enumerate(two): r.finish(rounder(way, gs, r.n, late))
        sq_all[0] = squares(late, n, total)
        swap = [pltpu.make_async_remote_copy(sq_all.at[0], sq_all.at[d], sq_send.at[d], sq_recv.at[d], device_id={axis: j}, device_id_type=MESH)
                for d, j in enumerate(others, 1)]
        for c in swap: c.start()
        for i, l, c, at, r in blocks_of(segs, 0, n):
            if r == LANES:
                gs[at:at + r, :] = gs[at:at + r, :].astype(F32).T.astype(BF)
        for c in swap: c.wait_recv()
        mean = jnp.sum(sq_all[:].sum(0), keepdims=True) / float(n * LANES * group)
        fac[:] = jnp.broadcast_to(jnp.minimum(1.0, 0.5 * lax.rsqrt(mean + 1e-30)), fac.shape)

        starts = sorted(at for _, _, _, at, _ in blocks_of(segs, 0, n)) + [n]
        cuts = [min(starts, key=lambda r: abs(r - n * t // (2 * parts))) for t in range(2 * parts + 1)]
        spans = list(zip(cuts, cuts[1:]))
        gathers = []
        for c in range(parts):
            for h in BOTH:
                span = spans[h * parts + c]
                for i, l, cs, at, r in blocks_of(segs, *span):
                    g = gs[at:at + r, :].astype(F32) * fac[0:1, :]
                    m, v = m_s[i][l, :, cs], v_s[i][l, :, cs] = moments(m_s[i][l, :, cs], v_s[i][l, :, cs], g)
                    w = w_s[i][l, :, cs].astype(F32)
                    new[at:at + r, :] = (w - lr * (m * lax.rsqrt(v + 1e-8) + 0.1 * w)).astype(BF)
                gathers.append(Gather(sq, h, c * 2 + h, span, new, buf, ag_send, ag_recv))
                gathers[-1].first()
        near, far = (1, 2), 3
        own = pltpu.make_async_copy(new, buf.at[me], own_sem)
        own.start()
        for x in gathers:
            x.pass_first()
            for b in near: x.second(b)
        for x in gathers: x.second(far)
        for x in gathers: x.pass_second(*near)
        for x in gathers: x.second(0)
        for x in gathers: x.pass_second(far)
        for x in gathers: x.pass_second(0)
        for x in gathers: x.end()
        own.wait()
        for c in swap: c.wait_send()


def tail(tokens, wide, low, sums, wo_part, weights, m, v, segs, n, axis, side, parts=3, bm=256):
    dq, _, _, h, *_ = tokens
    t, d = h.shape
    nh, _, hd = dq.shape
    k = len(m)
    group = side * side
    share = [a.shape for a in m]
    unit = share[0][1]
    n_big, n_small = wide.shape[2] * len(BOTH), (nh + 2) * unit
    n_wo = wo_part.shape[2]
    half, half_w = ((len(BOTH), side, x // len(BOTH), LANES) for x in (n_small, n_wo))
    out = [vm((group, n, LANES), BF)] + [vm(s, F32) for s in share] * 2
    room = [sd(a.shape, a.dtype) for a in out]
    return pl.pallas_call(
        functools.partial(_tail, axis=axis, side=side, segs=segs, parts=parts, lr=0.02), name="tail", grid=(t // bm,),
        out_shape=out, in_specs=pre_back_specs(nh, hd, d, bm) + [any_] * (len(sums) + 1 + 3 * k), out_specs=[any_] + [in_vmem] * (2 * k),
        scratch_shapes=[vm(s, BF) for s in share] +
                       [vm((d, (nh + 2) * hd), F32), vm((side, side, n_small, LANES), BF), vm((n, LANES), BF), vm((n, LANES), BF), sem_of(()), vm((group, 8, LANES), F32), vm((8, LANES), F32),
                        vm(half_w, F32), vm(half_w, BF), vm(half, F32), vm(half, BF), sem_of((3 * k,)), sem_of((2,)), sem_of((group,)), sem_of((group,)), *[sem_of((2 * parts, 5, 2, 2))] * 2] +
                       sum((ring_scratch(1, x, unit, F32) for x in (n_big, n_wo, n_small)), []) + sum((ring_scratch(side, x, unit, BF) for x in (n_wo, n_small)), []),
        compiler_params=params(room, **remote(4)),
    )(*tokens, wide, low, *sums, wo_part, *weights, *m, *v)


def _finish(buf_ref, *refs, segs, each):
    (m_in, v_in, w_out), refs = sevens(refs)
    k = len(m_in)
    outs, sem = refs[:-1], refs[-1]
    i = pl.program_id(0)
    stores = [pltpu.make_async_copy(a, b, sem.at[n]) for n, (a, b) in enumerate(zip((*m_in, *v_in), outs))]

    @on_first
    def _():
        for c in stores: c.start()

    for n in range(each):
        for a, l, c, at, r in blocks_of(segs, 0, buf_ref.shape[1]):
            w_out[a][l, n * r:n * r + r, c] = buf_ref[i * each + n, at:at + r, :]

    @on_last
    def _():
        for c in stores: c.wait()


def finish(buf, moments, weights, segs, each=2):
    k = len(moments)
    share = [a.shape for a in moments[:k // 2]]
    return pl.pallas_call(
        functools.partial(_finish, segs=segs, each=each), name="finish", grid=(buf.shape[0] // each,),
        in_specs=[in_vmem] * (1 + k), out_specs=[heads_block(a, b * each, c) for a, b, c in share] + [any_] * k,
        out_shape=[sd(w.shape, BF) for w in weights] + [sd(a.shape, F32) for a in moments],
        scratch_shapes=[sem_of((k,))],
        compiler_params=params([buf, *moments]),
    )(*map(stay, (buf, *moments)))


def solution(mesh):
    axis = "dp"
    group = mesh.shape[axis]
    side = round(group**0.5)

    def step(x, dy, *arrays):
        weights, m, v = (arrays[i : i + 7] for i in (0, 7, 14))
        wq, wk, wv, wo, *mlp = weights
        h0, dy = x[0], dy[0]
        qkv = wq, wk, wv
        head = wk.shape[2]
        scale = head**-0.5
        unit = m[0].shape[1]
        cos, sin = tables(h0.shape[0], head, THETA)
        q0, k0, v0 = pre(h0, cos, sin, *qkv, 0)
        o0, lse0 = attend(q0, k0, v0, scale)
        h1, gate_up, h2, q1, k1, v1 = middle(o0, h0, cos, sin, wo, *mlp, *qkv, 0)
        o1, lse1 = attend(q1, k1, v1, scale)
        dh, do, delta, big, small = mlp_back(o1, h2, dy, wo, *mlp, 1, side, axis, bm=512)
        d1 = attend_back(q1, k1, v1, do, lse1, delta, scale, big, side, axis, unit)
        dh, g1, small = pre_back(*d1, h2, cos, sin, 1, side, axis, small, dh, *qkv)
        _, do, delta, big, wo0, gw1 = mlp_back(o0, h1, dh, wo, *mlp, 0, side, axis, gate_up, small)
        *d0, wide, low = attend_back(q0, k0, v0, do, lse0, delta, scale, big, side, axis, unit)
        wq_, wk_, wv_, wo_, gate_, up_, down_ = range(7)
        order = [(i, l) for l in (1, 0) for i in (gate_, up_, down_, wo_, wq_, wk_, wv_)]
        segs, n = segments([w.shape for w in weights], order, group)
        buf, *moments = tail((*d0, h0, cos, sin), wide, low, (g1, gw1), wo0, weights, m, v, segs, n, axis, side)
        return tuple(finish(buf, moments, weights, segs))

    states, all_of, cut = P(("rep", "dp"), None, None), P(None, None, None), P(None, "dp", None)
    return jax.shard_map(
        step,
        mesh=mesh,
        in_specs=(states, states) + (all_of,) * 7 + (cut,) * 14,
        out_specs=(P("rep", None, None),) * 7 + (P("rep", "dp", None),) * 14,
        check_vma=False,
    )
```
